512 devices in a mesh: virt: 32 (over x, z), aux: 16 (over y, core).
Axes of the slice: x: 4, y: 8, z: 8, core: 2. Of those that a mesh axis runs over, the one named last changes fastest.
Arguments:
- three_index: bfloat16 [2400, 20480], P('aux', 'virt'), may hold values from -0.0625 to 0.0625
- eps_occ: float32 [20], replicated, may hold values from -1.5 to -0.5
- eps_virt: float32 [1024], replicated, may hold values from 0.3 to 3
Outputs:
- virt_energy: float32 [1024], P('virt')
- pair_energy: float32 [20, 20], replicated
The draws below stay inside these ranges and needn't reach their ends.
All inputs are finite; a program needn't handle non-finite values.
Results may differ from the reference program's by a relative error of at most 0.0003.
Values may be sent and summed in bfloat16 or wider, within the bound.
A program may use at most 128 MiB of HBM per device.

```python
import jax
import jax.numpy as jnp
from jax import lax

O = 20
VIRT_DEV = 32
VIRT = 1024
AUX = 2400


def level_of(own_key, shape, split, low, largest):
    gain = 1.0
    for axis_at, blocks in split:
        steps = jax.random.uniform(jax.random.fold_in(jax.random.fold_in(own_key, 6), axis_at), (blocks,), jnp.float32, low / len(split), largest / len(split))
        gain = gain * jnp.repeat(jnp.exp(steps), shape[axis_at] // blocks).reshape((-1,) + (1,) * (len(shape) - 1 - axis_at))
    return gain


def scatter_about(key, dims, spread, limit, split=(), kind=jnp.bfloat16):
    result = jax.random.normal(key, dims, jnp.float32) * spread
    if len(split) > 0:
        result = level_of(key, dims, split, -0.22, 0.18) * result
    return jnp.clip(result, min=-limit, max=limit).astype(kind)


def setup_inputs(seed: int = 0) -> dict:
    splits = jax.random.split(jax.random.key(seed), 4)
    three_index = scatter_about(splits[0], (AUX, VIRT * O), 0.011, 0.0625, ((0, 16), (1, 32)))
    eps_occ = jnp.clip(jax.random.uniform(splits[1], (O,), jnp.float32, -1.5, -0.5), -1.5, -0.5)
    eps_virt = jnp.clip(jax.random.uniform(splits[2], (VIRT,), jnp.float32, 0.3, 3.0), 0.3, 3.0)
    return {"three_index": three_index, "eps_occ": eps_occ, "eps_virt": eps_virt}


def reference(three_index, eps_occ, eps_virt):
    block_count = VIRT // VIRT_DEV
    widened = three_index.astype(jnp.float32).reshape(AUX, VIRT, O)

    def one_block(which):
        offset = (which * VIRT_DEV).astype(jnp.int32)
        left_rows = lax.dynamic_slice_in_dim(widened, offset, VIRT_DEV, 1)
        integrals = jnp.einsum("pai,pbj->iajb", left_rows, widened, precision=lax.Precision.HIGHEST)
        eps_own = lax.dynamic_slice_in_dim(eps_virt, offset, VIRT_DEV)
        denominator = (eps_occ[:, None, None, None] + eps_occ[None, None, :, None]
                       - eps_own[None, :, None, None] - eps_virt[None, None, None, :])
        swapped = jnp.transpose(integrals, (2, 1, 0, 3))
        energy_terms = integrals * (2.0 * integrals - swapped) / denominator
        return jnp.sum(energy_terms, axis=(0, 2, 3)), jnp.sum(energy_terms, axis=(1, 3))

    virt_parts, pair_parts = lax.map(one_block, jnp.arange(block_count, dtype=jnp.int32))
    return virt_parts.reshape(VIRT), jnp.sum(pair_parts, axis=0)
```

```python
import jax
import jax.numpy as jnp
from jax import lax
from jax.experimental import pallas as pl
from jax.experimental.pallas import tpu as pltpu
from jax.sharding import PartitionSpec as P

MESH = pl.DeviceIdType.MESH
BF = jnp.bfloat16
F32 = jnp.float32

O = 20
NX, NY, NZ = 4, 8, 8
ROWS, KP = 150, 160
AW = 640
NB = 4
SR = NB * O
KK = NY * KP
ORDER = (
    (0, 0), (0, 7), (3, 0), (1, 7), (0, 6), (2, 0), (1, 6), (3, 6), (2, 1),
    (1, 5), (3, 7), (2, 2), (2, 5), (0, 5), (1, 4), (0, 4), (1, 3), (2, 4),
)
SLOT = {d: n for n, d in enumerate(ORDER)}
HALF = ((0, 0), (0, 4), (2, 0), (2, 4))
NBLK = len(ORDER)
NPAIR = NBLK // 2
PARENT = (
    ((1, 6), (0, 6)), ((1, 4), (1, 5)), ((3, 0), (0, 0)), ((0, 5), (1, 5)), ((2, 4), (1, 4)),
    ((2, 5), (1, 5)), ((0, 4), (1, 4)), ((2, 1), (2, 0)), ((0, 6), (0, 7)), ((2, 2), (2, 1)),
    ((0, 7), (0, 0)), ((1, 5), (1, 6)), ((2, 0), (3, 0)), ((1, 7), (0, 7)), ((3, 6), (0, 6)),
    ((3, 7), (3, 6)), ((1, 3), (1, 4)),
)
CHILDREN = {}
for _child, _parent in PARENT:
    CHILDREN.setdefault(_parent, []).append(_child)
PIECES = ((0, 256), (256, 384), (640, 384), (1024, 256))
ARRIVALS = (
    (7.8, (0, 7), 0), (7.8, (3, 0), 0), (8.9, (0, 7), 1), (8.9, (3, 0), 1), (10.6, (0, 6), 0), (10.6, (1, 7), 0),
    (10.6, (2, 0), 0), (11.7, (1, 7), 1), (11.7, (0, 7), 2), (11.7, (3, 0), 2), (12.8, (0, 6), 1), (12.8, (2, 0), 1),
    (13.4, (1, 6), 0), (13.4, (2, 1), 0), (13.9, (0, 7), 3), (13.9, (3, 0), 3), (14.5, (1, 7), 2), (15.0, (3, 6), 0),
    (15.0, (0, 6), 2), (15.6, (1, 6), 1), (15.6, (2, 1), 1), (16.1, (2, 0), 2), (16.2, (1, 5), 0), (16.7, (2, 2), 0),
    (16.7, (1, 7), 3), (17.2, (3, 6), 1), (17.3, (0, 6), 3), (17.8, (3, 7), 0), (17.8, (1, 6), 2), (18.3, (2, 0), 3),
    (18.4, (1, 5), 1), (18.9, (2, 2), 1), (19.0, (2, 5), 0), (19.4, (3, 6), 2), (19.5, (1, 4), 0), (20.0, (2, 1), 2),
    (20.1, (1, 6), 3), (20.5, (0, 5), 0), (20.6, (1, 5), 2), (21.1, (3, 7), 1), (21.2, (2, 5), 1), (21.6, (3, 6), 3),
    (21.7, (1, 4), 1), (22.2, (2, 1), 3), (22.3, (2, 4), 0), (22.7, (0, 5), 1), (22.8, (1, 3), 0), (23.3, (3, 7), 2),
    (23.4, (2, 5), 2), (23.8, (0, 4), 0), (23.9, (1, 5), 3), (24.4, (2, 2), 2), (24.5, (2, 4), 1), (24.9, (0, 5), 2),
    (25.0, (1, 4), 2), (25.5, (3, 7), 3), (26.0, (0, 4), 1), (26.1, (1, 3), 1), (26.6, (2, 2), 3), (26.7, (2, 5), 3),
    (27.1, (0, 5), 3), (27.2, (1, 4), 3), (27.8, (2, 4), 2), (28.2, (0, 4), 2), (28.3, (1, 3), 2), (30.0, (0, 4), 3),
    (30.0, (1, 3), 3), (30.0, (2, 4), 3),
)
POS = {0: 0, 1: 1, 7: 2, 2: 3, 6: 4, 3: 5, 5: 6, 4: 7}
RING = tuple((1, n, h) for n in range(3) for h in range(2)) + ((1, 3, 0),)


def split_dot(a, b):
    high = a.astype(BF)
    rest = (a - high.astype(F32)).astype(BF)
    return jnp.dot(high, b, preferred_element_type=F32) + jnp.dot(rest, b, preferred_element_type=F32)


def iota(shape, axis):
    return lax.broadcasted_iota(jnp.int32, shape, axis)


def one_hot(mask):
    return jnp.where(mask, jnp.float32(1), jnp.float32(0)).astype(BF)


def swap_quads(block):
    rows, lanes = iota((16, 128), 0) // 4, iota((16, 128), 1) // 32
    result = block
    for k in range(1, 4):
        moved = pltpu.roll(pltpu.roll(block, 4 * k, 0), 128 - 32 * k, 1)
        result = jnp.where(((rows - lanes) & 3) == k, moved, result)
    return result


def kernel(
    x_ref, eo_ref, ev_ref, virt_ref, pair_ref,
    a_buf, slab, s_in, r_buf, c_buf, c_rx, eacc, row_e, lane_e, msg, rx1, msg2, rx2,
    a_send, a_recv, s_send, s_recv, r_send, r_recv, c_send, c_recv, f_send, f_recv, g_send, g_recv,
):
    w, u = lax.axis_index("virt"), lax.axis_index("aux")
    xx, zz = w // NZ, w % NZ
    yy, core = u // 2, u % 2

    def at_plane(dx, dz):
        return (xx + dx) % NX * NZ + (zz + dz) % NZ

    def at_line(dy, dc):
        return (yy + dy) % NY * 2 + (core + dc) % 2

    barrier = pltpu.get_barrier_semaphore()
    for e in range(1, NX * NZ):
        pl.semaphore_signal(barrier, inc=1, device_id=(at_plane(e // NZ, e % NZ), u), device_id_type=MESH)
    for e in range(1, 2 * NY):
        pl.semaphore_signal(barrier, inc=1, device_id=(w, at_line(e // 2, e % 2)), device_id_type=MESH)

    pad = one_hot(iota((KP, ROWS), 0) == iota((KP, ROWS), 1))
    own = jnp.dot(pad, x_ref[...], preferred_element_type=F32).astype(BF)
    for n in range(NY):
        lane = iota((AW, 128), 1)
        source = (4 * n + lane % 4) * O + lane // 4
        pick = one_hot((iota((AW, 128), 0) == source) & (lane < SR))
        slab[n] = jnp.dot(own, pick, preferred_element_type=F32).astype(BF)
    for n in range(AW // 128):
        lane = iota((AW, 128), 1) + 128 * n
        pick = one_hot(iota((AW, 128), 0) == lane % 32 * O + lane // 32)
        a_buf[0, :, 128 * n : 128 * n + 128] = jnp.dot(own, pick, preferred_element_type=F32).astype(BF)
    pl.semaphore_wait(barrier, NX * NZ - 1 + 2 * NY - 1)

    def slab_copy(delta):
        return pltpu.make_async_remote_copy(
            src_ref=slab.at[(yy + NY - delta) % NY], dst_ref=s_in.at[POS[delta]], send_sem=s_send,
            recv_sem=s_recv.at[POS[delta]], device_id=(w, at_line(NY - delta, 0)), device_id_type=MESH,
        )

    def ring_copy(step, delta, h):
        there = (delta + step) % NY
        rows = pl.ds(h * (KP // 2), KP // 2)
        return pltpu.make_async_remote_copy(
            src_ref=a_buf.at[POS[delta], rows], dst_ref=a_buf.at[POS[there], rows], send_sem=a_send,
            recv_sem=a_recv.at[POS[there], h], device_id=(w, at_line((NY - step) % NY, 0)), device_id_type=MESH,
        )

    def tree_copy(child, parent, piece):
        lanes = pl.ds(*PIECES[piece])
        step = ((parent[0] - child[0]) % NX, (parent[1] - child[1]) % NZ)
        return pltpu.make_async_remote_copy(
            src_ref=r_buf.at[SLOT[parent], :, lanes], dst_ref=r_buf.at[SLOT[child], :, lanes], send_sem=r_send,
            recv_sem=r_recv.at[SLOT[child], piece], device_id=(at_plane(*step), u), device_id_type=MESH,
        )

    for delta in (1, 7, 2, 6, 3, 5, 4):
        slab_copy(delta).start()
    for h in range(2):
        ring_copy(1, 0, h).start()
        ring_copy(7, 0, h).start()
    s_in[0] = slab[yy]

    quad_b = iota((8, 128), 0) % 4
    for n in range(O // 2):
        top = iota((8, 128), 0) < 4
        row_e[8 * n : 8 * n + 8] = jnp.where(top, eo_ref[2 * n], eo_ref[2 * n + 1])
    own_v = jnp.zeros((8, 128), F32)
    lane32 = iota((8, 128), 1) % 32
    for a in range(32):
        own_v = jnp.where(lane32 == a, ev_ref[w * 32 + a], own_v)
    for n in range(AW // 128):
        group = iota((8, 128), 1) // 32
        occ = jnp.full((8, 128), eo_ref[4 * n], F32)
        for r in range(1, 4):
            occ = jnp.where(group == r, eo_ref[4 * n + r], occ)
        lane_e[:, 128 * n : 128 * n + 128] = occ - own_v
    eacc[...] = jnp.zeros_like(eacc)
    msg[...] = jnp.zeros_like(msg)

    eye = one_hot(iota((SR, 128), 0) == iota((SR, 128), 1))

    def turn(first, count):
        rows = s_in[first : first + count].reshape(count * KP, 128)
        return lax.dot_general(eye, rows, (((1,), (1,)), ((), ())), preferred_element_type=F32).astype(BF)

    def pass_on(block, piece):
        for child in CHILDREN.get(block, ()):
            tree_copy(child, block, piece).start()

    for pos in range(1, 4):
        slab_copy([d for d in POS if POS[d] == pos][0]).wait_recv()
    r_buf[0, :, 0:640] = turn(0, 4)
    pass_on((0, 0), 0)
    pass_on((0, 0), 1)
    for pos in range(4, 8):
        slab_copy([d for d in POS if POS[d] == pos][0]).wait_recv()
    r_buf[0, :, 640:1280] = turn(4, 4)
    pass_on((0, 0), 2)
    pass_on((0, 0), 3)

    def core_copy(p):
        return pltpu.make_async_remote_copy(
            src_ref=c_buf.at[p, 1 - core], dst_ref=c_rx.at[p], send_sem=c_send, recv_sem=c_recv.at[p],
            device_id=(w, at_line(0, 1)), device_id_type=MESH,
        )

    def multiply(p):
        rows = r_buf[2 * p : 2 * p + 2].reshape(2 * SR, KK)
        product = jnp.dot(rows, a_buf[...].reshape(KK, AW), preferred_element_type=F32)
        c_buf[p, 0] = product[:SR]
        c_buf[p, 1] = product[SR:]
        core_copy(p).start()

    def finish(p):
        core_copy(p).wait_recv()
        c_rx[p] = c_rx[p] + c_buf[p, core]
        (x0, z0), (x1, z1) = ORDER[2 * p], ORDER[2 * p + 1]
        other = at_plane(x0 + core * (x1 - x0), z0 + core * (z1 - z0))
        w0, w1 = (0.5 if d in HALF else 1.0 for d in ORDER[2 * p : 2 * p + 2])
        weight = jnp.where(core == 0, jnp.float32(w0), jnp.float32(w1))
        minus = jnp.zeros((8, 128), F32)
        for b in range(NB):
            minus = jnp.where(quad_b == b, ev_ref[other * 32 + yy * NB + b], minus)
        minus = jnp.concatenate([minus, minus], 0)
        shares = jnp.zeros((16, 128), F32)
        for q in range(5):
            rows = slice(16 * q, 16 * q + 16)
            part = row_e[rows] - minus
            for l in range(5):
                lanes = slice(128 * l, 128 * l + 128)
                value = c_rx[p, rows, lanes]
                swapped = swap_quads(c_rx[p, 16 * l : 16 * l + 16, 128 * q : 128 * q + 128])
                lane = lane_e[:, lanes]
                term = value * (2.0 * value - swapped) * (weight / (part + jnp.concatenate([lane, lane], 0)))
                eacc[rows, lanes] += term
                shares += term
        shares = shares[:8] + shares[8:]
        total = jnp.sum(shares, axis=1, keepdims=True)
        start = 64 if p < 8 else 96
        spread = jnp.where(iota((8, 128), 1) == start + yy * NB + quad_b, total, 0.0)
        line = jnp.sum(spread, axis=0, keepdims=True)
        msg[...] += jnp.where(iota((8, 128), 0) == p % 8, line, 0.0)

    events = [(t, "r", (b, piece)) for t, b, piece in ARRIVALS]
    for n in range(1, 8):
        delta, h = (n + 1) // 2, (n + 1) % 2
        events.append((8.7 + 2.2 * n, "a", (1, delta, h)))
        events.append((8.7 + 2.2 * n, "a", (7, NY - delta, h if delta < 4 else 1)))
    events.sort(key=lambda e: e[0])
    left_a = 14
    pieces = {(0, 0): 4}
    done = finished = 0

    def advance(limit):
        nonlocal done, finished
        steps = 0
        while (
            steps < limit and left_a == 0 and done < NPAIR
            and all(pieces.get(d, 0) == 4 for d in ORDER[2 * done : 2 * done + 2])
        ):
            multiply(done)
            done += 1
            if done >= 2:
                finish(finished)
                finished += 1
            steps += 1

    for _, kind, what in events:
        if kind == "a":
            step, delta, h = what
            before = (delta - step) % NY
            ring_copy(step, before, h).wait_recv()
            if delta not in (4,) and ((delta + step) % NY != 4 or h == (0 if step == 1 else 1)):
                ring_copy(step, delta, h).start()
            left_a -= 1
        else:
            block, piece = what
            parent = dict(PARENT)[block]
            tree_copy(block, parent, piece).wait_recv()
            pass_on(block, piece)
            pieces[block] = pieces.get(block, 0) + 1
        advance(1)
    advance(NPAIR)
    while finished < NPAIR:
        finish(finished)
        finished += 1

    total = eacc[...]
    lane = iota((AW, 128), 1)
    pick = one_hot((iota((AW, 128), 0) // 32 == lane % O) & (lane < 3 * O))
    summed = split_dot(total, pick)
    row, lane = iota((SR, 128), 0), iota((SR, 128), 1)
    summed = jnp.where(row // 32 == lane // O, summed, 0.0)
    fold = one_hot(iota((8, SR), 0) == iota((8, SR), 1) // 4 % 8)
    high = summed.astype(BF)
    rest = (summed - high.astype(F32)).astype(BF)
    packed = jnp.dot(fold, high, preferred_element_type=F32) + jnp.dot(fold, rest, preferred_element_type=F32)
    msg[...] += packed
    for e in range(1, NX * NZ):
        pltpu.make_async_remote_copy(
            src_ref=msg, dst_ref=rx1.at[e], send_sem=f_send, recv_sem=f_recv,
            device_id=(at_plane(e // NZ, e % NZ), u), device_id_type=MESH,
        ).start()
    own = total[:, 0:128]
    for n in range(1, 5):
        own = own + total[:, 128 * n : 128 * n + 128]
    own = jnp.sum(own, axis=0, keepdims=True)
    own = own + pltpu.roll(own, 64, 1)
    own = own + pltpu.roll(own, 32, 1)

    pltpu.make_async_copy(rx1.at[1:], rx1.at[1:], f_recv).wait()
    row, lane = iota((8, 128), 0), iota((8, 128), 1)
    pairs = msg[...]
    low = jnp.zeros((8, 128), F32)
    high = jnp.zeros((8, 128), F32)
    for e in range(NX * NZ):
        got = msg[...] if e == 0 else rx1[e]
        if e:
            pairs = pairs + got
        n = SLOT.get((e // NZ, e % NZ))
        if n is not None:
            mine = (row == n // 2 % 8) & (core == n % 2)
            if n // 2 < 8:
                low = low + jnp.where(mine, got, 0.0)
            else:
                high = high + jnp.where(mine, got, 0.0)
    low = jnp.sum(low, axis=0, keepdims=True)
    high = jnp.sum(high, axis=0, keepdims=True)
    shares = own + low + pltpu.roll(high, 96, 1)
    msg2[...] = jnp.where(lane < 64, pairs, jnp.where(row == 0, shares, 0.0))
    for e in range(1, 2 * NY):
        pltpu.make_async_remote_copy(
            src_ref=msg2, dst_ref=rx2.at[e], send_sem=g_send, recv_sem=g_recv,
            device_id=(w, at_line(NY - e // 2, e % 2)), device_id_type=MESH,
        ).start()
    pltpu.make_async_copy(rx2.at[1:], rx2.at[1:], g_recv).wait()
    total = msg2[...]
    for e in range(1, 2 * NY):
        total = total + rx2[e]
    virt_ref[...] = pltpu.roll(total, 64, 1)[0:1, 0:32]
    wide = jnp.concatenate(
        [total, pltpu.roll(total, 128 - O, 1), pltpu.roll(total, 128 - 2 * O, 1), jnp.zeros((104, 128), F32)], 0
    )
    pair_ref[...] = (wide + jnp.transpose(wide))[:O, :O]

    def drain(ref, sem):
        pltpu.make_async_copy(ref, ref, sem).wait()

    drain(s_in.at[1:], s_send)
    drain(a_buf.at[1:], a_send)
    drain(r_buf.at[1:], r_send)
    drain(c_rx, c_send)
    drain(rx1.at[1:], f_send)
    drain(rx2.at[1:], g_send)


def on_device(three_index, eps_occ, eps_virt):
    vmem, smem = pl.BlockSpec(memory_space=pltpu.VMEM), pl.BlockSpec(memory_space=pltpu.SMEM)
    dma = pltpu.SemaphoreType.DMA
    virt, pair = pl.pallas_call(
        kernel,
        out_shape=(jax.ShapeDtypeStruct((1, 32), F32), jax.ShapeDtypeStruct((O, O), F32)),
        in_specs=[vmem, smem, smem],
        out_specs=(vmem, vmem),
        scratch_shapes=[
            pltpu.VMEM((NY, KP, AW), BF),
            pltpu.VMEM((NY, KP, 128), BF),
            pltpu.VMEM((NY, KP, 128), BF),
            pltpu.VMEM((NBLK, SR, KK), BF),
            pltpu.VMEM((NPAIR, 2, SR, AW), F32),
            pltpu.VMEM((NPAIR, SR, AW), F32),
            pltpu.VMEM((SR, AW), F32),
            pltpu.VMEM((SR, 128), F32),
            pltpu.VMEM((8, AW), F32),
            pltpu.VMEM((8, 128), F32),
            pltpu.VMEM((NX * NZ, 8, 128), F32),
            pltpu.VMEM((8, 128), F32),
            pltpu.VMEM((2 * NY, 8, 128), F32),
            dma, dma((NY, 2)), dma, dma((NY,)), dma, dma((NBLK, 4)), dma, dma((NPAIR,)),
            dma, dma, dma, dma,
        ],
        compiler_params=pltpu.CompilerParams(collective_id=0, has_side_effects=True, vmem_limit_bytes=56 * 1024 * 1024),
        name="mp2",
    )(three_index, eps_occ, eps_virt)
    return virt.reshape(32), pair


def solution(mesh):
    return jax.shard_map(
        on_device, mesh=mesh, in_specs=(P("aux", "virt"), P(), P()), out_specs=(P("virt"), P()), check_vma=False
    )
```

```python
import jax
import jax.numpy as jnp
from jax import lax
from jax.experimental import pallas as pl
from jax.experimental.pallas import tpu as pltpu
from jax.sharding import PartitionSpec as P

MESH = pl.DeviceIdType.MESH
BF = jnp.bfloat16
F32 = jnp.float32

O = 20
NX, NY, NZ = 4, 8, 8
ROWS, KP = 150, 160
AW = 640
NB = 4
SR = NB * O
KK = NY * KP
GR = 56
ORDER = (
    (0, 0), (3, 0), (3, 1), (3, 7), (0, 1), (2, 1), (3, 2), (3, 6), (0, 2),
    (3, 3), (2, 2), (2, 0), (0, 3), (3, 4), (2, 3), (3, 5), (2, 4), (0, 4),
)
SLOT = {d: n for n, d in enumerate(ORDER)}
HALF = ((0, 0), (0, 4), (2, 0), (2, 4))
NBLK = len(ORDER)
NPAIR = NBLK // 2
TREE = {
    (3, 0): (((0, 0), 6.4), ((0, 0), 8.7), ((0, 0), 9.6), ((0, 0), 10.5), ((0, 0), 11.4)),
    (3, 1): (((3, 0), 9.6), ((3, 0), 11.6), ((3, 0), 13.4), ((0, 1), 14.1), ((3, 0), 14.3)),
    (3, 7): (((3, 0), 9.3), ((3, 0), 11.6), ((3, 0), 13.4), ((3, 0), 14.3), ((3, 0), 15.2)),
    (0, 1): (((0, 0), 6.4), ((0, 0), 8.7), ((3, 1), 16.3), ((0, 0), 10.5), ((3, 1), 17.2)),
    (2, 1): (((3, 1), 13.2), ((3, 1), 15.0), ((3, 1), 16.8), ((3, 1), 17.7), ((3, 1), 18.6)),
    (3, 2): (((3, 1), 12.5), ((3, 1), 15.2), ((3, 1), 17.0), ((3, 1), 17.9), ((3, 1), 18.8)),
    (3, 6): (((3, 7), 12.5), ((3, 7), 16.1), ((3, 7), 18.8), ((3, 7), 19.7), ((3, 7), 20.6)),
    (0, 2): (((3, 2), 15.4), ((3, 2), 18.1), ((3, 2), 19.9), ((3, 2), 20.8), ((3, 2), 21.7)),
    (3, 3): (((3, 2), 16.1), ((3, 2), 19.7), ((3, 2), 20.6), ((3, 2), 21.5), ((3, 2), 22.4)),
    (2, 2): (((3, 2), 15.9), ((3, 2), 19.5), ((3, 2), 21.3), ((3, 2), 22.2), ((3, 2), 23.1)),
    (2, 0): (((2, 1), 17.9), ((3, 0), 12.3), ((2, 1), 22.4), ((2, 1), 24.2), ((2, 1), 25.1)),
    (0, 3): (((3, 3), 19.0), ((3, 3), 22.6), ((3, 3), 23.5), ((3, 3), 24.4), ((3, 3), 25.3)),
    (3, 4): (((3, 5), 23.3), ((3, 3), 23.3), ((3, 5), 28.9), ((3, 3), 25.1), ((3, 3), 26.0)),
    (2, 3): (((3, 3), 20.4), ((3, 3), 24.0), ((3, 3), 24.9), ((3, 3), 25.8), ((3, 3), 26.7)),
    (3, 5): (((3, 6), 17.0), ((3, 6), 21.5), ((3, 6), 26.0), ((3, 6), 26.9), ((3, 6), 27.8)),
    (2, 4): (((2, 3), 24.2), ((2, 3), 27.8), ((2, 3), 28.7), ((3, 4), 28.0), ((3, 4), 28.9)),
    (0, 4): (((3, 4), 26.2), ((3, 4), 27.1), ((0, 3), 26.9), ((3, 4), 28.0), ((3, 4), 28.9)),
}
PIECES = 5
PW = KK // PIECES
POS = {0: 0, 1: 1, 7: 2, 2: 3, 6: 4, 3: 5, 5: 6, 4: 7}
DELTA = {n: d for d, n in POS.items()}
NEAR = 768
A_AFTER = 5
A_START, A_STEP, LATE = 9.0, 2.2, 1.5


def hops(dx, dz, dy):
    return min(dx, NX - dx) + min(dz, NZ - dz) + min(dy, NY - dy)


PLANE = sorted(range(1, NX * NZ), key=lambda e: -hops(e // NZ, e % NZ, 0))
LINE = sorted(range(1, 2 * NY), key=lambda e: -hops(0, 0, e // 2))


def passed_on(block, piece):
    return [child for child, row in TREE.items() if row[piece][0] == block]


def program_order():
    forward, arrival = [], {((0, 0), n): 0.0 for n in range(PIECES)}
    for block, row in TREE.items():
        for piece, (_, t) in enumerate(row):
            arrival[block, piece] = t
            if passed_on(block, piece):
                forward.append((t, ("r", block, piece)))
    ring = [A_START + A_STEP * n for n in range(8)]
    for n in range(1, 7):
        delta, h = (n + 1) // 2, (n + 1) % 2
        for step, d in ((1, delta), (7, NY - delta)):
            if delta < 3 or h == (0 if step == 1 else 1):
                forward.append((ring[n], ("a", step, d, h)))
    forward.sort(key=lambda e: e[0])
    tasks = []
    for p in range(NPAIR):
        both = ORDER[2 * p : 2 * p + 2]
        first = max([ring[4]] + [arrival[b, n] for b in both for n in range(3)])
        second = max([ring[7]] + [arrival[b, n] for b in both for n in range(PIECES)])
        tasks += [[first + LATE, 0.35, ("m", p, 0)], [second + LATE, 0.25, ("m", p, 1)], [second + LATE + 1.6, 0.35, ("f", p)]]
    tasks.sort(key=lambda e: e[0])
    steps, t = [], 0.0
    while forward or tasks:
        if not tasks or forward and max(t, tasks[0][0]) + tasks[0][1] > forward[0][0]:
            when, what = forward.pop(0)
            t = max(t, when)
        else:
            ready, length, what = tasks.pop(0)
            t = max(t, ready) + length
            for task in tasks:
                if task[2] == ("f", what[1]):
                    task[0] = max(task[0], t + 1.6)
            tasks.sort(key=lambda e: e[0])
        steps.append(what)
    return steps


def split_dot(a, b):
    high = a.astype(BF)
    rest = (a - high.astype(F32)).astype(BF)
    return jnp.dot(high, b, preferred_element_type=F32) + jnp.dot(rest, b, preferred_element_type=F32)


def iota(shape, axis):
    return lax.broadcasted_iota(jnp.int32, shape, axis)


def one_hot(mask):
    return jnp.where(mask, jnp.float32(1), jnp.float32(0)).astype(BF)


def swap_quads(block):
    rows, lanes = iota((16, 128), 0) // 4, iota((16, 128), 1) // 32
    result = block
    for k in range(1, 4):
        moved = pltpu.roll(pltpu.roll(block, 4 * k, 0), 128 - 32 * k, 1)
        result = jnp.where(((rows - lanes) & 3) == k, moved, result)
    return result


def groups(block, moves):
    return [pltpu.roll(rows, m, 1) if m else rows for rows, m in zip(block, moves)]


def pack(block):
    parts = block[:GR], block[GR : 2 * GR], jnp.concatenate([block[2 * GR :], jnp.zeros((3 * GR - KP, 128), F32)], 0)
    lane = iota((GR, 128), 1)
    halves = []
    for moves in ((0, 40, 80), (88, 0, 40)):
        first, second, third = groups(parts, moves)
        halves.append(jnp.where(lane < 40, first, jnp.where(lane < 80, second, third)))
    return jnp.concatenate(halves, 0)


def unpack(block):
    low, high = block[:GR], block[GR:]
    lane = iota((GR, 128), 1)
    parts = []
    for moves in ((0, 40), (88, 0), (48, 88)):
        first, second = groups((low, high), moves)
        parts.append(jnp.where(lane < 40, first, second))
    return jnp.concatenate([parts[0], parts[1], parts[2][: KP - 2 * GR]], 0)


def kernel(
    x_ref, eo_ref, ev_ref, sum_ref,
    a_buf, slab, s_in, s_all, r_buf, c_buf, c_rx, eacc, row_e, lane_e, msg, rx1, msg2, rx2,
    a_send, a_recv, s_send, s_recv, r_send, r_recv, c_send, c_recv, f_send, f_recv, g_send, g_recv,
):
    w, u = lax.axis_index("virt"), lax.axis_index("aux")
    xx, zz = w // NZ, w % NZ
    yy, core = u // 2, u % 2

    def at_plane(dx, dz):
        return (xx + dx) % NX * NZ + (zz + dz) % NZ

    def at_line(dy, dc):
        return (yy + dy) % NY * 2 + (core + dc) % 2

    barrier = pltpu.get_barrier_semaphore()
    for e in PLANE:
        pl.semaphore_signal(barrier, inc=1, device_id=(at_plane(e // NZ, e % NZ), u), device_id_type=MESH)
    for e in LINE:
        pl.semaphore_signal(barrier, inc=1, device_id=(w, at_line(e // 2, e % 2)), device_id_type=MESH)

    pad = one_hot(iota((KP, ROWS), 0) == iota((KP, ROWS), 1))
    own = jnp.dot(pad, x_ref[...], preferred_element_type=F32).astype(BF)
    for n in range(0, NY, 2):
        lane = iota((AW, 256), 1)
        inner = lane & 127
        upper = jnp.where(inner < 40, 0, 1)
        source = (4 * n + 4 * (lane // 128) + 2 * upper + (inner & 1)) * O + (inner - 40 * upper) // 2
        pick = one_hot((iota((AW, 256), 0) == source) & (inner < SR))
        both = jnp.dot(own, pick, preferred_element_type=F32)
        slab[n] = pack(both[:, :128]).astype(BF)
        slab[n + 1] = pack(both[:, 128:]).astype(BF)
    with jax.named_scope("barrier"):
        pl.semaphore_wait(barrier, NX * NZ - 1 + 2 * NY - 1)

    def slab_copy(delta):
        return pltpu.make_async_remote_copy(
            src_ref=slab.at[(yy + NY - delta) % NY], dst_ref=s_in.at[POS[delta]], send_sem=s_send,
            recv_sem=s_recv.at[POS[delta]], device_id=(w, at_line(NY - delta, 0)), device_id_type=MESH,
        )

    def ring_copy(step, delta, h):
        there = (delta + step) % NY
        half = KP // 2
        return pltpu.make_async_remote_copy(
            src_ref=a_buf.at[pl.ds(POS[delta] * KP + h * half, half)],
            dst_ref=a_buf.at[pl.ds(POS[there] * KP + h * half, half)], send_sem=a_send,
            recv_sem=a_recv.at[POS[there], h], device_id=(w, at_line((NY - step) % NY, 0)), device_id_type=MESH,
        )

    def tree_copy(child, piece):
        parent = TREE[child][piece][0]
        lanes = pl.ds(piece * PW, PW)
        step = ((parent[0] - child[0]) % NX, (parent[1] - child[1]) % NZ)
        return pltpu.make_async_remote_copy(
            src_ref=r_buf.at[SLOT[parent], :, lanes], dst_ref=r_buf.at[SLOT[child], :, lanes], send_sem=r_send,
            recv_sem=r_recv.at[SLOT[child], piece], device_id=(at_plane(*step), u), device_id_type=MESH,
        )

    for delta in (1, 7, 2, 6, 3, 5, 4):
        slab_copy(delta).start()
    s_all[0:KP] = unpack(slab[yy].astype(F32)).astype(BF)

    for first, width in ((0, 256), (256, 256), (512, 128)):
        lane = iota((AW, width), 1) + first
        pick = one_hot(iota((AW, width), 0) == (lane & 31) * O + lane // 32)
        a_buf[0:KP, first : first + width] = jnp.dot(own, pick, preferred_element_type=F32).astype(BF)

    row = iota((SR, 128), 0)
    eye = one_hot(iota((SR, 128), 1) == (row // 2 & 1) * 40 + row // 4 * 2 + (row & 1))
    known = 0
    for piece in range(PIECES):
        need = min(((piece + 1) * PW - 1) // KP, NY - 1)
        while known < need:
            known += 1
            with jax.named_scope(f"slab_wait{known}"):
                slab_copy(DELTA[known]).wait_recv()
            s_all[known * KP : known * KP + KP] = unpack(s_in[known].astype(F32)).astype(BF)
            if known == A_AFTER:
                for h in range(2):
                    ring_copy(1, 0, h).start()
                    ring_copy(7, 0, h).start()
        lanes = slice(piece * PW, piece * PW + PW)
        turned = lax.dot_general(eye, s_all[lanes], (((1,), (1,)), ((), ())), preferred_element_type=F32)
        r_buf[0, :, lanes] = turned.astype(BF)
        for child in passed_on((0, 0), piece):
            tree_copy(child, piece).start()

    quad_b = iota((8, 128), 0) & 3
    for n in range(O // 2):
        top = iota((8, 128), 0) < 4
        row_e[8 * n : 8 * n + 8] = jnp.where(top, eo_ref[2 * n], eo_ref[2 * n + 1])
    own_v = jnp.zeros((8, 128), F32)
    lane32 = iota((8, 128), 1) & 31
    for a in range(32):
        own_v = jnp.where(lane32 == a, ev_ref[w * 32 + a], own_v)
    for n in range(AW // 128):
        group = iota((8, 128), 1) // 32
        occ = jnp.full((8, 128), eo_ref[4 * n], F32)
        for r in range(1, 4):
            occ = jnp.where(group == r, eo_ref[4 * n + r], occ)
        lane_e[:, 128 * n : 128 * n + 128] = occ - own_v
    eacc[...] = jnp.zeros_like(eacc)
    msg[...] = jnp.zeros_like(msg)

    def core_copy(p):
        return pltpu.make_async_remote_copy(
            src_ref=c_buf.at[p, 1 - core], dst_ref=c_rx.at[p], send_sem=c_send, recv_sem=c_recv.at[p],
            device_id=(w, at_line(0, 1)), device_id_type=MESH,
        )

    seen = {("r", (0, 0), n) for n in range(PIECES)} | {("a", 0, 0), ("a", 0, 1)}

    def wait_tree(block, piece):
        if ("r", block, piece) not in seen:
            seen.add(("r", block, piece))
            with jax.named_scope(f"r{block[0]}{block[1]}_{piece}"):
                tree_copy(block, piece).wait_recv()

    def wait_ring(delta, h):
        if ("a", delta, h) not in seen:
            seen.add(("a", delta, h))
            step = 1 if delta < 4 or delta == 4 and h == 0 else 7
            with jax.named_scope(f"a{delta}_{h}"):
                ring_copy(step, (delta - step) % NY, h).wait_recv()

    def multiply(p, half):
        for n in range(3) if half == 0 else range(3, PIECES):
            wait_tree(ORDER[2 * p], n)
            wait_tree(ORDER[2 * p + 1], n)
        for pos in range(5 if half == 0 else NY):
            for h in range(2):
                wait_ring(DELTA[pos], h)
        part = slice(0, NEAR) if half == 0 else slice(NEAR, KK)
        rows = r_buf[2 * p : 2 * p + 2, :, part].reshape(2 * SR, part.stop - part.start)
        product = jnp.dot(rows, a_buf[part], preferred_element_type=F32)
        if half == 0:
            c_buf[p, 0] = product[:SR]
            c_buf[p, 1] = product[SR:]
        else:
            c_buf[p, 0] += product[:SR]
            c_buf[p, 1] += product[SR:]
            core_copy(p).start()

    def finish(p):
        with jax.named_scope(f"c_wait{p}"):
            core_copy(p).wait_recv()
        c_rx[p] = c_rx[p] + c_buf[p, core]
        (x0, z0), (x1, z1) = ORDER[2 * p], ORDER[2 * p + 1]
        other = at_plane(x0 + core * (x1 - x0), z0 + core * (z1 - z0))
        w0, w1 = (0.5 if d in HALF else 1.0 for d in ORDER[2 * p : 2 * p + 2])
        weight = jnp.where(core == 0, jnp.float32(w0), jnp.float32(w1))
        minus = jnp.zeros((8, 128), F32)
        for b in range(NB):
            minus = jnp.where(quad_b == b, ev_ref[other * 32 + yy * NB + b], minus)
        minus = jnp.concatenate([minus, minus], 0)
        shares = jnp.zeros((16, 128), F32)
        for q in range(5):
            rows = slice(16 * q, 16 * q + 16)
            part = row_e[rows] - minus
            for l in range(5):
                lanes = slice(128 * l, 128 * l + 128)
                value = c_rx[p, rows, lanes]
                swapped = swap_quads(c_rx[p, 16 * l : 16 * l + 16, 128 * q : 128 * q + 128])
                lane = lane_e[:, lanes]
                term = value * (2.0 * value - swapped) * (weight / (part + jnp.concatenate([lane, lane], 0)))
                eacc[rows, lanes] += term
                shares += term
        shares = shares[:8] + shares[8:]
        total = jnp.sum(shares[:4] + shares[4:], axis=1, keepdims=True)
        msg[...] += jnp.where(iota((4, 128), 1) == 100 + p, total, 0.0)

    for step in program_order():
        if step[0] == "a":
            _, way, delta, h = step
            wait_ring(delta, h)
            ring_copy(way, delta, h).start()
        elif step[0] == "r":
            _, block, piece = step
            wait_tree(block, piece)
            for child in passed_on(block, piece):
                tree_copy(child, piece).start()
        else:
            with jax.named_scope("_".join(map(str, step))):
                multiply(*step[1:]) if step[0] == "m" else finish(*step[1:])

    total = eacc[...]
    lane = iota((AW, 128), 1)
    pick = one_hot((iota((AW, 128), 0) // 32 == lane % O) & (lane < 5 * O))
    summed = split_dot(total, pick)
    row, lane = iota((SR, 128), 0), iota((SR, 128), 1)
    summed = jnp.where(row // 16 == lane // O, summed, 0.0)
    fold = one_hot(iota((8, SR), 0) == (iota((8, SR), 1) // 4 & 3))
    high = summed.astype(BF)
    rest = (summed - high.astype(F32)).astype(BF)
    packed = jnp.dot(fold, high, preferred_element_type=F32) + jnp.dot(fold, rest, preferred_element_type=F32)
    msg[...] += packed[:4]
    for e in PLANE:
        pltpu.make_async_remote_copy(
            src_ref=msg, dst_ref=rx1.at[e], send_sem=f_send, recv_sem=f_recv,
            device_id=(at_plane(e // NZ, e % NZ), u), device_id_type=MESH,
        ).start()
    own = total[:, 0:128]
    for n in range(1, 5):
        own = own + total[:, 128 * n : 128 * n + 128]
    own = jnp.sum(own, axis=0, keepdims=True)
    own = own + pltpu.roll(own, 64, 1)
    own = own + pltpu.roll(own, 32, 1)
    row, lane = iota((4, 128), 0), iota((4, 128), 1)
    tail = jnp.zeros((4, 128), F32)
    for r in range(4):
        tail = jnp.where(row == r, pltpu.roll(own, 100 - 8 * r, 1), tail)

    with jax.named_scope("f_wait"):
        pltpu.make_async_copy(rx1.at[1:], rx1.at[1:], f_recv).wait()
    pairs = msg[...]
    theirs = jnp.zeros((4, 128), F32)
    for e in range(NX * NZ):
        got = msg[...] if e == 0 else rx1[e]
        if e:
            pairs = pairs + got
        n = SLOT.get((e // NZ, e % NZ))
        if n is not None:
            theirs = theirs + jnp.where((lane == 100 + n // 2) & (core == n % 2), got, 0.0)
    theirs = jnp.sum(theirs, axis=1, keepdims=True)
    theirs = jnp.where(lane == 100 + (yy & 1) * NB + row, theirs, 0.0)
    theirs = jnp.sum(theirs, axis=0, keepdims=True)
    tail = tail + jnp.where(row == yy // 2, theirs, 0.0)
    msg2[...] = jnp.where(lane < 100, pairs, tail)
    for e in LINE:
        pltpu.make_async_remote_copy(
            src_ref=msg2, dst_ref=rx2.at[e], send_sem=g_send, recv_sem=g_recv,
            device_id=(w, at_line(NY - e // 2, e % 2)), device_id_type=MESH,
        ).start()
    with jax.named_scope("g_wait"):
        pltpu.make_async_copy(rx2.at[1:], rx2.at[1:], g_recv).wait()
    total = msg2[...]
    for e in range(1, 2 * NY):
        total = total + rx2[e]
    sum_ref[...] = total

    def drain(ref, sem):
        pltpu.make_async_copy(ref, ref, sem).wait()

    drain(s_in.at[1:], s_send)
    drain(a_buf.at[KP:], a_send)
    drain(r_buf.at[1:], r_send)
    drain(c_rx, c_send)
    drain(rx1.at[1:], f_send)
    drain(rx2.at[1:], g_send)


def open_sums(sum_ref, virt_ref, pair_ref, square):
    total = sum_ref[...]
    row, lane = iota((4, 128), 0), iota((4, 128), 1)
    line = jnp.zeros((4, 128), F32)
    for r in range(4):
        line = jnp.where((row == r) & (lane // 8 == r), pltpu.roll(total, 28 + 8 * r, 1), line)
    virt_ref[...] = jnp.sum(line, axis=0)[:32]
    square[...] = jnp.zeros_like(square)
    for q in range(5):
        square[4 * q : 4 * q + 4] = pltpu.roll(total, (128 - O * q) % 128, 1)
    wide = square[...]
    pair_ref[...] = (wide + jnp.transpose(wide))[:O, :O]


def on_device(three_index, eps_occ, eps_virt):
    vmem, smem = pl.BlockSpec(memory_space=pltpu.VMEM), pl.BlockSpec(memory_space=pltpu.SMEM)
    dma = pltpu.SemaphoreType.DMA
    sums = pl.pallas_call(
        kernel,
        out_shape=jax.ShapeDtypeStruct((4, 128), F32),
        in_specs=[vmem, smem, smem],
        out_specs=vmem,
        scratch_shapes=[
            pltpu.VMEM((KK, AW), BF),
            pltpu.VMEM((NY, 2 * GR, 128), BF),
            pltpu.VMEM((NY, 2 * GR, 128), BF),
            pltpu.VMEM((KK, 128), BF),
            pltpu.VMEM((NBLK, SR, KK), BF),
            pltpu.VMEM((NPAIR, 2, SR, AW), F32),
            pltpu.VMEM((NPAIR, SR, AW), F32),
            pltpu.VMEM((SR, AW), F32),
            pltpu.VMEM((SR, 128), F32),
            pltpu.VMEM((8, AW), F32),
            pltpu.VMEM((4, 128), F32),
            pltpu.VMEM((NX * NZ, 4, 128), F32),
            pltpu.VMEM((4, 128), F32),
            pltpu.VMEM((2 * NY, 4, 128), F32),
            dma, dma((NY, 2)), dma, dma((NY,)), dma, dma((NBLK, PIECES)), dma, dma((NPAIR,)),
            dma, dma, dma, dma,
        ],
        compiler_params=pltpu.CompilerParams(collective_id=0, has_side_effects=True, vmem_limit_bytes=56 * 1024 * 1024),
        name="mp2",
    )(three_index, eps_occ, eps_virt)
    return pl.pallas_call(
        open_sums,
        out_shape=(jax.ShapeDtypeStruct((32,), F32), jax.ShapeDtypeStruct((O, O), F32)),
        in_specs=[vmem],
        out_specs=(vmem, vmem),
        scratch_shapes=[pltpu.VMEM((128, 128), F32)],
        name="sums",
    )(sums)


def solution(mesh):
    return jax.shard_map(
        on_device, mesh=mesh, in_specs=(P("aux", "virt"), P(), P()), out_specs=(P("virt"), P()), check_vma=False
    )
```

```python
import jax
import jax.numpy as jnp
from jax import lax
from jax.experimental import pallas as pl
from jax.experimental.pallas import tpu as pltpu
from jax.sharding import PartitionSpec as P

MESH = pl.DeviceIdType.MESH
BF = jnp.bfloat16
F32 = jnp.float32

O = 20
NX, NY, NZ = 4, 8, 8
ROWS, KP = 150, 160
AW = 640
NB = 4
SR = NB * O
KK = NY * KP
GR = 56
ORDER = (
    (0, 0), (1, 0), (0, 1), (3, 1), (2, 0), (0, 2), (2, 7), (3, 2), (0, 3),
    (2, 6), (3, 7), (3, 3), (0, 4), (2, 5), (3, 6), (3, 4), (2, 4), (3, 5),
)
SLOT = {d: n for n, d in enumerate(ORDER)}
HALF = ((0, 0), (0, 4), (2, 0), (2, 4))
NBLK = len(ORDER)
NPAIR = NBLK // 2
TREE = {
    (1, 0): (((0, 0), 6.8), ((0, 0), 9.2), ((0, 0), 11.0), ((0, 0), 13.2), ((0, 0), 14.1)),
    (0, 1): (((0, 0), 6.8), ((0, 0), 9.2), ((0, 0), 11.0), ((0, 0), 13.2), ((0, 0), 15.0)),
    (3, 1): (((3, 2), 17.2), ((0, 1), 12.3), ((0, 1), 14.1), ((0, 1), 16.3), ((0, 1), 18.1)),
    (2, 0): (((1, 0), 10.1), ((1, 0), 12.3), ((1, 0), 15.0), ((1, 0), 16.3), ((1, 0), 18.1)),
    (0, 2): (((0, 1), 10.1), ((0, 1), 12.3), ((0, 1), 15.9), ((0, 1), 17.7), ((0, 1), 18.6)),
    (2, 7): (((2, 0), 13.2), ((2, 0), 15.4), ((2, 0), 18.1), ((2, 0), 19.9), ((2, 0), 21.2)),
    (3, 2): (((0, 2), 13.2), ((0, 2), 15.4), ((0, 2), 19.0), ((0, 2), 20.8), ((0, 2), 21.7)),
    (0, 3): (((0, 2), 14.1), ((0, 2), 16.8), ((0, 2), 19.5), ((0, 2), 21.3), ((0, 2), 22.2)),
    (2, 6): (((2, 7), 16.3), ((2, 7), 19.0), ((2, 7), 22.1), ((2, 7), 23.0), ((2, 7), 24.3)),
    (3, 7): (((2, 7), 17.2), ((2, 7), 19.0), ((2, 7), 21.2), ((2, 7), 23.0), ((2, 7), 24.8)),
    (3, 3): (((0, 3), 17.2), ((0, 3), 19.9), ((0, 3), 22.6), ((0, 3), 24.4), ((0, 3), 25.3)),
    (0, 4): (((3, 4), 23.9), ((3, 4), 27.5), ((0, 3), 23.1), ((0, 3), 25.8), ((0, 3), 26.7)),
    (2, 5): (((3, 5), 28.0), ((2, 4), 30.2), ((2, 6), 25.2), ((2, 6), 26.1), ((2, 6), 27.4)),
    (3, 6): (((2, 6), 19.9), ((2, 6), 22.1), ((2, 6), 25.7), ((2, 6), 26.6), ((3, 7), 28.3)),
    (3, 4): (((3, 3), 20.4), ((3, 3), 24.0), ((0, 4), 26.2), ((0, 4), 28.9), ((3, 3), 28.5)),
    (2, 4): (((3, 4), 23.5), ((3, 4), 27.1), ((3, 4), 29.8), ((2, 5), 29.2), ((2, 5), 30.5)),
    (3, 5): (((3, 4), 24.9), ((3, 4), 27.6), ((2, 5), 28.4), ((2, 5), 29.3), ((2, 5), 30.5)),
}
BOUNDS = (0, 256, 512, 768, 1024, 1280)
PIECES = len(BOUNDS) - 1
POS = {0: 0, 1: 1, 7: 2, 2: 3, 6: 4, 3: 5, 5: 6, 4: 7}
DELTA = {n: d for d, n in POS.items()}
PARTS = (0, 768, KK)
A_AFTER = 3
A_PARTS = 5
LATE, SLACK, GAP = 0.7, 0.5, 3.5
SLABS = (0.0, 3.3, 4.2, 5.8, 6.8, 8.5, 8.9, 9.8)

RING = {
    1: (8.9, 9.8, 10.7, 11.6, 12.5, 13.4, 14.3, 15.2, 16.1, 17.0, 17.9, 18.8, 19.7, 20.6, 21.5, 22.4, 23.3, 24.2),
    7: (8.9, 9.8, 10.7, 11.6, 12.5, 13.4, 14.3, 15.2, 16.1, 17.0, 17.9, 18.8, 19.7, 20.6, 21.5, 22.4, 23.3),
}


def hops(dx, dz, dy):
    return min(dx, NX - dx) + min(dz, NZ - dz) + min(dy, NY - dy)


PLANE = sorted(range(1, NX * NZ), key=lambda e: -hops(e // NZ, e % NZ, 0))
LINE = sorted(range(1, 2 * NY), key=lambda e: -hops(0, 0, e // 2))


def passed_on(block, piece):
    return [child for child, row in TREE.items() if row[piece][0] == block]


def ring_pieces(step):
    last = range(3) if step == 1 else range(3, A_PARTS)
    return [(step * n % NY, h) for n in range(1, 4) for h in range(A_PARTS)] + [(4, h) for h in last]


def ring_goes_on(step, delta, h):
    return ((delta + step) % NY, h) in ring_pieces(step)


def part_needs(first, last):
    pieces = [m for m in range(PIECES) if BOUNDS[m] < last and BOUNDS[m + 1] > first]
    return pieces, range(first // KP, (last - 1) // KP + 1)


def program_order():
    forward, arrival = [], {((0, 0), n): 0.0 for n in range(PIECES)}
    for block, row in TREE.items():
        for piece, (_, t) in enumerate(row):
            arrival[block, piece] = t
            if passed_on(block, piece):
                forward.append((t, ("r", block, piece)))
    forward += [(t, ("s", pos)) for pos, t in enumerate(SLABS) if pos]
    rings = {}
    for step, times in RING.items():
        for (delta, h), t in zip(ring_pieces(step), times):
            rings[delta, h] = t
            if ring_goes_on(step, delta, h):
                forward.append((t, ("a", step, delta, h)))
    forward.sort(key=lambda e: e[0])
    tasks = [[0.0, 0.25, ("d", p)] for p in range(NPAIR)]
    last = max(rings.values())
    for p in range(NPAIR):
        both = ORDER[2 * p : 2 * p + 2]
        early = max(arrival[b, m] for b in both for m in range(PIECES)) < last - 1.0
        bounds = PARTS if early else (0, KK)
        ready = 0.0
        for a, b in zip(bounds, bounds[1:]):
            pieces, chunks = part_needs(a, b)
            times = [arrival[d, m] for d in both for m in pieces]
            times += [rings[DELTA[m], h] for m in chunks if m for h in range(A_PARTS)]
            ready = max([ready] + times)
            tasks.append([ready + LATE, 0.2 + 0.25 * (b - a) / KK, ("m", p, a, b)])
        tasks.append([ready + LATE + GAP, 0.25, ("f", p)])
    tasks.sort(key=lambda e: e[0])
    steps, t = [], 0.0
    while forward or tasks:
        if not tasks or forward and max(t, tasks[0][0]) + tasks[0][1] > forward[0][0] + SLACK:
            when, what = forward.pop(0)
            t = max(t, when)
        else:
            ready, length, what = tasks.pop(0)
            t = max(t, ready) + length
            for task in tasks:
                if what[0] == "m" and task[2] == ("f", what[1]):
                    task[0] = max(task[0], t + GAP)
            tasks.sort(key=lambda e: e[0])
        steps.append(what)
    return steps


def split_dot(a, b):
    high = a.astype(BF)
    rest = (a - high.astype(F32)).astype(BF)
    return jnp.dot(high, b, preferred_element_type=F32) + jnp.dot(rest, b, preferred_element_type=F32)


def iota(shape, axis):
    return lax.broadcasted_iota(jnp.int32, shape, axis)


def one_hot(mask):
    return jnp.where(mask, jnp.float32(1), jnp.float32(0)).astype(BF)


def swap_quads(block):
    row, lane = iota((8, 128), 0) // 4, iota((8, 128), 1) // 32
    far = lane // 2
    top = jnp.where(far == 0, block[:8], pltpu.roll(block[8:], 64, 1))
    bottom = jnp.where(far == 1, block[8:], pltpu.roll(block[:8], 64, 1))
    near = lane & 1
    result = []
    for part in (top, bottom):
        turned = pltpu.roll(part, 4, 0)
        moved = jnp.where(near == 1, pltpu.roll(turned, 32, 1), pltpu.roll(turned, 96, 1))
        result.append(jnp.where(near == row, part, moved))
    return jnp.concatenate(result, 0)


def groups(block, moves):
    return [pltpu.roll(rows, m, 1) if m else rows for rows, m in zip(block, moves)]


def pack(block):
    parts = block[:GR], block[GR : 2 * GR], jnp.concatenate([block[2 * GR :], jnp.zeros((3 * GR - KP, 128), F32)], 0)
    lane = iota((GR, 128), 1)
    halves = []
    for moves in ((0, 40, 80), (88, 0, 40)):
        first, second, third = groups(parts, moves)
        halves.append(jnp.where(lane < 40, first, jnp.where(lane < 80, second, third)))
    return jnp.concatenate(halves, 0)


def unpack(block):
    low, high = block[:GR], block[GR:]
    lane = iota((GR, 128), 1)
    parts = []
    for moves in ((0, 40), (88, 0), (48, 88)):
        first, second = groups((low, high), moves)
        parts.append(jnp.where(lane < 40, first, second))
    return jnp.concatenate([parts[0], parts[1], parts[2][: KP - 2 * GR]], 0)


def kernel(
    x_ref, eo_ref, ev_ref, sum_ref,
    a_buf, slab, s_in, s_all, r_buf, c_buf, c_rx, factor, eacc, row_e, lane_e, msg, rx1, msg2, rx2,
    a_send, a_recv, s_send, s_recv, r_send, r_recv, c_send, c_recv, f_send, f_recv, g_send, g_recv,
):
    w, u = lax.axis_index("virt"), lax.axis_index("aux")
    xx, zz = w // NZ, w % NZ
    yy, core = u // 2, u % 2

    def at_plane(dx, dz):
        return (xx + dx) % NX * NZ + (zz + dz) % NZ

    def at_line(dy, dc):
        return (yy + dy) % NY * 2 + (core + dc) % 2

    barrier = pltpu.get_barrier_semaphore()
    for e in PLANE:
        pl.semaphore_signal(barrier, inc=1, device_id=(at_plane(e // NZ, e % NZ), u), device_id_type=MESH)
    for e in LINE:
        pl.semaphore_signal(barrier, inc=1, device_id=(w, at_line(e // 2, e % 2)), device_id_type=MESH)

    pad = one_hot(iota((KP, ROWS), 0) == iota((KP, ROWS), 1))
    own = jnp.dot(pad, x_ref[...], preferred_element_type=F32).astype(BF)
    for n in range(0, NY, 2):
        lane = iota((AW, 256), 1)
        inner = lane & 127
        upper = jnp.where(inner < 40, 0, 1)
        source = (4 * n + 4 * (lane // 128) + 2 * upper + (inner & 1)) * O + (inner - 40 * upper) // 2
        pick = one_hot((iota((AW, 256), 0) == source) & (inner < SR))
        both = jnp.dot(own, pick, preferred_element_type=F32)
        slab[n] = pack(both[:, :128]).astype(BF)
        slab[n + 1] = pack(both[:, 128:]).astype(BF)
    with jax.named_scope("barrier"):
        pl.semaphore_wait(barrier, NX * NZ - 1 + 2 * NY - 1)

    def slab_copy(delta):
        return pltpu.make_async_remote_copy(
            src_ref=slab.at[(yy + NY - delta) % NY], dst_ref=s_in.at[POS[delta]], send_sem=s_send,
            recv_sem=s_recv.at[POS[delta]], device_id=(w, at_line(NY - delta, 0)), device_id_type=MESH,
        )

    def ring_copy(step, delta, h):
        there = (delta + step) % NY
        part = KP // A_PARTS
        return pltpu.make_async_remote_copy(
            src_ref=a_buf.at[pl.ds(POS[delta] * KP + h * part, part)],
            dst_ref=a_buf.at[pl.ds(POS[there] * KP + h * part, part)], send_sem=a_send,
            recv_sem=a_recv.at[POS[there], h], device_id=(w, at_line((NY - step) % NY, 0)), device_id_type=MESH,
        )

    def tree_copy(child, piece):
        parent = TREE[child][piece][0]
        lanes = pl.ds(BOUNDS[piece], BOUNDS[piece + 1] - BOUNDS[piece])
        step = ((parent[0] - child[0]) % NX, (parent[1] - child[1]) % NZ)
        return pltpu.make_async_remote_copy(
            src_ref=r_buf.at[SLOT[parent], :, lanes], dst_ref=r_buf.at[SLOT[child], :, lanes], send_sem=r_send,
            recv_sem=r_recv.at[SLOT[child], piece], device_id=(at_plane(*step), u), device_id_type=MESH,
        )

    for delta in (1, 7, 2, 6, 3, 5, 4):
        slab_copy(delta).start()
    s_all[0:KP] = unpack(slab[yy].astype(F32)).astype(BF)

    row = iota((SR, 128), 0)
    eye = one_hot(iota((SR, 128), 1) == (row // 2 & 1) * 40 + row // 4 * 2 + (row & 1))
    def own_piece(piece):
        lanes = slice(BOUNDS[piece], BOUNDS[piece + 1])
        turned = lax.dot_general(eye, s_all[lanes], (((1,), (1,)), ((), ())), preferred_element_type=F32)
        r_buf[0, :, lanes] = turned.astype(BF)
        for child in passed_on((0, 0), piece):
            tree_copy(child, piece).start()

    def take_slab(pos):
        with jax.named_scope(f"slab_wait{pos}"):
            slab_copy(DELTA[pos]).wait_recv()
        s_all[pos * KP : pos * KP + KP] = unpack(s_in[pos].astype(F32)).astype(BF)
        for piece in range(PIECES):
            if (BOUNDS[piece + 1] - 1) // KP == pos:
                own_piece(piece)
        if pos == A_AFTER:
            for h in range(A_PARTS):
                ring_copy(1, 0, h).start()
                ring_copy(7, 0, h).start()

    if BOUNDS[1] <= KP:
        own_piece(0)

    for first, width in ((0, 256), (256, 256), (512, 128)):
        lane = iota((AW, width), 1) + first
        pick = one_hot(iota((AW, width), 0) == (lane & 31) * O + lane // 32)
        a_buf[0:KP, first : first + width] = jnp.dot(own, pick, preferred_element_type=F32).astype(BF)

    quad_b = iota((8, 128), 0) & 3
    for n in range(O // 2):
        top = iota((8, 128), 0) < 4
        row_e[8 * n : 8 * n + 8] = jnp.where(top, eo_ref[2 * n], eo_ref[2 * n + 1])
    own_v = jnp.zeros((8, 128), F32)
    lane32 = iota((8, 128), 1) & 31
    for a in range(32):
        own_v = jnp.where(lane32 == a, ev_ref[w * 32 + a], own_v)
    for n in range(AW // 128):
        group = iota((8, 128), 1) // 32
        occ = jnp.full((8, 128), eo_ref[4 * n], F32)
        for r in range(1, 4):
            occ = jnp.where(group == r, eo_ref[4 * n + r], occ)
        lane_e[:, 128 * n : 128 * n + 128] = occ - own_v
    eacc[...] = jnp.zeros_like(eacc)
    msg[...] = jnp.zeros_like(msg)

    def core_copy(p):
        return pltpu.make_async_remote_copy(
            src_ref=c_buf.at[p, 1 - core], dst_ref=c_rx.at[p], send_sem=c_send, recv_sem=c_recv.at[p],
            device_id=(w, at_line(0, 1)), device_id_type=MESH,
        )

    seen = {("r", (0, 0), n) for n in range(PIECES)} | {("a", 0, h) for h in range(A_PARTS)}

    def wait_tree(block, piece):
        if ("r", block, piece) not in seen:
            seen.add(("r", block, piece))
            with jax.named_scope(f"r{block[0]}{block[1]}_{piece}"):
                tree_copy(block, piece).wait_recv()

    def wait_ring(delta, h):
        if ("a", delta, h) not in seen:
            seen.add(("a", delta, h))
            step = 1 if (delta, h) in ring_pieces(1) else 7
            with jax.named_scope(f"a{delta}_{h}"):
                ring_copy(step, (delta - step) % NY, h).wait_recv()

    def multiply(p, first, last):
        pieces, chunks = part_needs(first, last)
        for m in pieces:
            wait_tree(ORDER[2 * p], m)
            wait_tree(ORDER[2 * p + 1], m)
        for m in chunks:
            for h in range(A_PARTS):
                wait_ring(DELTA[m], h)
        part = slice(first, last)
        rows = r_buf[2 * p : 2 * p + 2, :, part].reshape(2 * SR, last - first)
        product = jnp.dot(rows, a_buf[part], preferred_element_type=F32)
        if first == 0:
            c_buf[p, 0] = product[:SR]
            c_buf[p, 1] = product[SR:]
        else:
            c_buf[p, 0] += product[:SR]
            c_buf[p, 1] += product[SR:]
        if last == KK:
            core_copy(p).start()

    def divide(p):
        (x0, z0), (x1, z1) = ORDER[2 * p], ORDER[2 * p + 1]
        other = at_plane(x0 + core * (x1 - x0), z0 + core * (z1 - z0))
        w0, w1 = (0.5 if d in HALF else 1.0 for d in ORDER[2 * p : 2 * p + 2])
        weight = jnp.where(core == 0, jnp.float32(w0), jnp.float32(w1))
        minus = jnp.zeros((8, 128), F32)
        for b in range(NB):
            minus = jnp.where(quad_b == b, ev_ref[other * 32 + yy * NB + b], minus)
        for q in range(10):
            rows = slice(8 * q, 8 * q + 8)
            part = row_e[rows] - minus
            for l in range(5):
                lanes = slice(128 * l, 128 * l + 128)
                factor[p, rows, lanes] = weight / (part + lane_e[:, lanes])

    def finish(p):
        with jax.named_scope(f"c_wait{p}"):
            core_copy(p).wait_recv()
        c_rx[p] = c_rx[p] + c_buf[p, core]
        shares = jnp.zeros((16, 128), F32)
        for q in range(5):
            rows = slice(16 * q, 16 * q + 16)
            for l in range(5):
                lanes = slice(128 * l, 128 * l + 128)
                value = c_rx[p, rows, lanes]
                inner = 2.0 * value
                if l >= q:
                    swapped = swap_quads(c_rx[p, 16 * l : 16 * l + 16, 128 * q : 128 * q + 128])
                    inner = inner - swapped if l == q else 2.0 * (value - swapped)
                term = value * inner * factor[p, rows, lanes]
                eacc[rows, lanes] += term
                shares += term
        shares = shares[:8] + shares[8:]
        total = jnp.sum(shares[:4] + shares[4:], axis=1, keepdims=True)
        msg[...] += jnp.where(iota((4, 128), 1) == 100 + p, total, 0.0)

    for step in program_order():
        if step[0] == "s":
            take_slab(step[1])
        elif step[0] == "a":
            _, way, delta, h = step
            wait_ring(delta, h)
            ring_copy(way, delta, h).start()
        elif step[0] == "r":
            _, block, piece = step
            wait_tree(block, piece)
            for child in passed_on(block, piece):
                tree_copy(child, piece).start()
        else:
            with jax.named_scope("_".join(map(str, step))):
                {"m": multiply, "f": finish, "d": divide}[step[0]](*step[1:])

    total = eacc[...]
    lane = iota((AW, 128), 1)
    pick = one_hot((iota((AW, 128), 0) // 32 == lane % O) & (lane < 5 * O))
    summed = split_dot(total, pick)
    row, lane = iota((SR, 128), 0), iota((SR, 128), 1)
    summed = jnp.where(row // 16 == lane // O, summed, 0.0)
    fold = one_hot(iota((8, SR), 0) == (iota((8, SR), 1) // 4 & 3))
    high = summed.astype(BF)
    rest = (summed - high.astype(F32)).astype(BF)
    packed = jnp.dot(fold, high, preferred_element_type=F32) + jnp.dot(fold, rest, preferred_element_type=F32)
    msg[...] += packed[:4]
    for e in PLANE:
        pltpu.make_async_remote_copy(
            src_ref=msg, dst_ref=rx1.at[e], send_sem=f_send, recv_sem=f_recv,
            device_id=(at_plane(e // NZ, e % NZ), u), device_id_type=MESH,
        ).start()
    own = total[:, 0:128]
    for n in range(1, 5):
        own = own + total[:, 128 * n : 128 * n + 128]
    own = jnp.sum(own, axis=0, keepdims=True)
    own = own + pltpu.roll(own, 64, 1)
    own = own + pltpu.roll(own, 32, 1)
    row, lane = iota((4, 128), 0), iota((4, 128), 1)
    tail = jnp.zeros((4, 128), F32)
    for r in range(4):
        tail = jnp.where(row == r, pltpu.roll(own, 100 - 8 * r, 1), tail)

    def drain(ref, sem):
        pltpu.make_async_copy(ref, ref, sem).wait()

    drain(s_in.at[1:], s_send)
    drain(a_buf.at[KP:], a_send)
    drain(r_buf.at[1:], r_send)
    drain(c_rx, c_send)
    with jax.named_scope("f_wait"):
        pltpu.make_async_copy(rx1.at[1:], rx1.at[1:], f_recv).wait()
    pairs = msg[...]
    theirs = jnp.zeros((4, 128), F32)
    for e in range(NX * NZ):
        got = msg[...] if e == 0 else rx1[e]
        if e:
            pairs = pairs + got
        n = SLOT.get((e // NZ, e % NZ))
        if n is not None:
            theirs = theirs + jnp.where((lane == 100 + n // 2) & (core == n % 2), got, 0.0)
    theirs = jnp.sum(theirs, axis=1, keepdims=True)
    theirs = jnp.where(lane == 100 + (yy & 1) * NB + row, theirs, 0.0)
    theirs = jnp.sum(theirs, axis=0, keepdims=True)
    tail = tail + jnp.where(row == yy // 2, theirs, 0.0)
    msg2[...] = jnp.where(lane < 100, pairs, tail)
    for e in LINE:
        pltpu.make_async_remote_copy(
            src_ref=msg2, dst_ref=rx2.at[e], send_sem=g_send, recv_sem=g_recv,
            device_id=(w, at_line(NY - e // 2, e % 2)), device_id_type=MESH,
        ).start()
    with jax.named_scope("g_wait"):
        pltpu.make_async_copy(rx2.at[1:], rx2.at[1:], g_recv).wait()
    total = msg2[...]
    for e in range(1, 2 * NY):
        total = total + rx2[e]
    sum_ref[...] = total

    drain(rx1.at[1:], f_send)
    drain(rx2.at[1:], g_send)


def open_sums(sum_ref, virt_ref, pair_ref, square):
    total = sum_ref[...]
    row, lane = iota((4, 128), 0), iota((4, 128), 1)
    line = jnp.zeros((4, 128), F32)
    for r in range(4):
        line = jnp.where((row == r) & (lane // 8 == r), pltpu.roll(total, 28 + 8 * r, 1), line)
    virt_ref[...] = jnp.sum(line, axis=0)[:32]
    square[...] = jnp.zeros_like(square)
    for q in range(5):
        square[4 * q : 4 * q + 4] = pltpu.roll(total, (128 - O * q) % 128, 1)
    wide = square[...]
    pair_ref[...] = (wide + jnp.transpose(wide))[:O, :O]


def on_device(three_index, eps_occ, eps_virt):
    vmem, smem = pl.BlockSpec(memory_space=pltpu.VMEM), pl.BlockSpec(memory_space=pltpu.SMEM)
    dma = pltpu.SemaphoreType.DMA
    sums = pl.pallas_call(
        kernel,
        out_shape=jax.ShapeDtypeStruct((4, 128), F32),
        in_specs=[vmem, smem, smem],
        out_specs=vmem,
        scratch_shapes=[
            pltpu.VMEM((KK, AW), BF),
            pltpu.VMEM((NY, 2 * GR, 128), BF),
            pltpu.VMEM((NY, 2 * GR, 128), BF),
            pltpu.VMEM((KK, 128), BF),
            pltpu.VMEM((NBLK, SR, KK), BF),
            pltpu.VMEM((NPAIR, 2, SR, AW), F32),
            pltpu.VMEM((NPAIR, SR, AW), F32),
            pltpu.VMEM((NPAIR, SR, AW), F32),
            pltpu.VMEM((SR, AW), F32),
            pltpu.VMEM((SR, 128), F32),
            pltpu.VMEM((8, AW), F32),
            pltpu.VMEM((4, 128), F32),
            pltpu.VMEM((NX * NZ, 4, 128), F32),
            pltpu.VMEM((4, 128), F32),
            pltpu.VMEM((2 * NY, 4, 128), F32),
            dma, dma((NY, A_PARTS)), dma, dma((NY,)), dma, dma((NBLK, PIECES)), dma, dma((NPAIR,)),
            dma, dma, dma, dma,
        ],
        compiler_params=pltpu.CompilerParams(collective_id=0, has_side_effects=True, vmem_limit_bytes=56 * 1024 * 1024),
        name="mp2",
    )(three_index, eps_occ, eps_virt)
    return pl.pallas_call(
        open_sums,
        out_shape=(jax.ShapeDtypeStruct((32,), F32), jax.ShapeDtypeStruct((O, O), F32)),
        in_specs=[vmem],
        out_specs=(vmem, vmem),
        scratch_shapes=[pltpu.VMEM((128, 128), F32)],
        name="sums",
    )(sums)


def solution(mesh):
    return jax.shard_map(
        on_device, mesh=mesh, in_specs=(P("aux", "virt"), P(), P()), out_specs=(P("virt"), P()), check_vma=False
    )
```

```python
import jax
import jax.numpy as jnp
from jax import lax
from jax.experimental import pallas as pl
from jax.experimental.pallas import tpu as pltpu
from jax.sharding import PartitionSpec as P

MESH = pl.DeviceIdType.MESH
BF = jnp.bfloat16
F32 = jnp.float32

O = 20
NX, NY, NZ = 4, 8, 8
ROWS, KP = 150, 160
AW = 640
NB = 4
SR = NB * O
KK = NY * KP
GR = 56
ORDER = (
    (0, 0), (1, 0), (0, 1), (3, 1), (2, 0), (0, 2), (2, 7), (3, 2), (0, 3),
    (2, 6), (3, 7), (3, 3), (0, 4), (2, 5), (3, 6), (3, 4), (2, 4), (3, 5),
)
SLOT = {d: n for n, d in enumerate(ORDER)}
HALF = ((0, 0), (0, 4), (2, 0), (2, 4))
NBLK = len(ORDER)
NPAIR = NBLK // 2
TREE = {
    (1, 0): (((0, 0), 6.8), ((0, 0), 9.2), ((0, 0), 11.0), ((0, 0), 13.2), ((0, 0), 14.1)),
    (0, 1): (((0, 0), 6.8), ((0, 0), 9.2), ((0, 0), 11.0), ((0, 0), 13.2), ((0, 0), 15.0)),
    (3, 1): (((3, 2), 17.2), ((0, 1), 12.3), ((0, 1), 14.1), ((0, 1), 16.3), ((0, 1), 18.1)),
    (2, 0): (((1, 0), 10.1), ((1, 0), 12.3), ((1, 0), 15.0), ((1, 0), 16.3), ((1, 0), 18.1)),
    (0, 2): (((0, 1), 10.1), ((0, 1), 12.3), ((0, 1), 15.9), ((0, 1), 17.7), ((0, 1), 18.6)),
    (2, 7): (((2, 0), 13.2), ((2, 0), 15.4), ((2, 0), 18.1), ((2, 0), 19.9), ((2, 0), 21.2)),
    (3, 2): (((0, 2), 13.2), ((0, 2), 15.4), ((0, 2), 19.0), ((0, 2), 20.8), ((0, 2), 21.7)),
    (0, 3): (((0, 2), 14.1), ((0, 2), 16.8), ((0, 2), 19.5), ((0, 2), 21.3), ((0, 2), 22.2)),
    (2, 6): (((2, 7), 16.3), ((2, 7), 19.0), ((2, 7), 22.1), ((2, 7), 23.0), ((2, 7), 24.3)),
    (3, 7): (((2, 7), 17.2), ((2, 7), 19.0), ((2, 7), 21.2), ((2, 7), 23.0), ((2, 7), 24.8)),
    (3, 3): (((0, 3), 17.2), ((0, 3), 19.9), ((0, 3), 22.6), ((0, 3), 24.4), ((0, 3), 25.3)),
    (0, 4): (((3, 4), 23.9), ((3, 4), 27.5), ((0, 3), 23.1), ((0, 3), 25.8), ((0, 3), 26.7)),
    (2, 5): (((3, 5), 28.0), ((2, 4), 30.2), ((2, 6), 25.2), ((2, 6), 26.1), ((2, 6), 27.4)),
    (3, 6): (((2, 6), 19.9), ((2, 6), 22.1), ((2, 6), 25.7), ((2, 6), 26.6), ((3, 7), 28.3)),
    (3, 4): (((3, 3), 20.4), ((3, 3), 24.0), ((0, 4), 26.2), ((0, 4), 28.9), ((3, 3), 28.5)),
    (2, 4): (((3, 4), 23.5), ((3, 4), 27.1), ((3, 4), 29.8), ((2, 5), 29.2), ((2, 5), 30.5)),
    (3, 5): (((3, 4), 24.9), ((3, 4), 27.6), ((2, 5), 28.4), ((2, 5), 29.3), ((2, 5), 30.5)),
}
BOUNDS = (0, 256, 512, 768, 1024, 1280)
PIECES = len(BOUNDS) - 1
POS = {0: 0, 1: 1, 7: 2, 2: 3, 6: 4, 3: 5, 5: 6, 4: 7}
DELTA = {n: d for d, n in POS.items()}
PARTS = (0, 768, KK)
A_AFTER = 3
A_PARTS = 5
LATE, SLACK, GAP = 0.7, 0.5, 3.5
SLABS = (0.0, 3.3, 4.2, 5.8, 6.8, 8.5, 8.9, 9.8)

RING = {
    1: (8.9, 9.8, 10.7, 11.6, 12.5, 13.4, 14.3, 15.2, 16.1, 17.0, 17.9, 18.8, 19.7, 20.6, 21.5, 22.4, 23.3, 24.2),
    7: (8.9, 9.8, 10.7, 11.6, 12.5, 13.4, 14.3, 15.2, 16.1, 17.0, 17.9, 18.8, 19.7, 20.6, 21.5, 22.4, 23.3),
}


def hops(dx, dz, dy):
    return min(dx, NX - dx) + min(dz, NZ - dz) + min(dy, NY - dy)


PLANE = sorted(range(1, NX * NZ), key=lambda e: -hops(e // NZ, e % NZ, 0))
NEXT = [e for e in PLANE if hops(e // NZ, e % NZ, 0) == 1]
LINE = sorted(range(1, 2 * NY), key=lambda e: -hops(0, 0, e // 2))


def passed_on(block, piece):
    return [child for child, row in TREE.items() if row[piece][0] == block]


def ring_pieces(step):
    last = range(3) if step == 1 else range(3, A_PARTS)
    return [(step * n % NY, h) for n in range(1, 4) for h in range(A_PARTS)] + [(4, h) for h in last]


def ring_goes_on(step, delta, h):
    return ((delta + step) % NY, h) in ring_pieces(step)


def part_needs(first, last):
    pieces = [m for m in range(PIECES) if BOUNDS[m] < last and BOUNDS[m + 1] > first]
    return pieces, range(first // KP, (last - 1) // KP + 1)


def program_order():
    forward, arrival = [], {((0, 0), n): 0.0 for n in range(PIECES)}
    for block, row in TREE.items():
        for piece, (_, t) in enumerate(row):
            arrival[block, piece] = t
            if piece == 0 or passed_on(block, piece):
                forward.append((t, ("r", block, piece)))
    forward += [(t, ("s", pos)) for pos, t in enumerate(SLABS) if pos]
    rings = {}
    for step, times in RING.items():
        for (delta, h), t in zip(ring_pieces(step), times):
            rings[delta, h] = t
            if ring_goes_on(step, delta, h):
                forward.append((t, ("a", step, delta, h)))
    forward.sort(key=lambda e: e[0])
    tasks = [[0.0, 0.25, ("d", p)] for p in range(NPAIR)]
    last = max(rings.values())
    for p in range(NPAIR):
        both = ORDER[2 * p : 2 * p + 2]
        early = max(arrival[b, m] for b in both for m in range(PIECES)) < last - 1.0
        bounds = PARTS if early else (0, KK)
        ready = 0.0
        for a, b in zip(bounds, bounds[1:]):
            pieces, chunks = part_needs(a, b)
            times = [arrival[d, m] for d in both for m in pieces]
            times += [rings[DELTA[m], h] for m in chunks if m for h in range(A_PARTS)]
            ready = max([ready] + times)
            tasks.append([ready + LATE, 0.2 + 0.25 * (b - a) / KK, ("m", p, a, b)])
        tasks.append([ready + LATE + GAP, 0.25, ("f", p)])
    tasks.sort(key=lambda e: e[0])
    steps, t = [], 0.0
    while forward or tasks:
        if not tasks or forward and max(t, tasks[0][0]) + tasks[0][1] > forward[0][0] + SLACK:
            when, what = forward.pop(0)
            t = max(t, when)
        else:
            ready, length, what = tasks.pop(0)
            t = max(t, ready) + length
            for task in tasks:
                if what[0] == "m" and task[2] == ("f", what[1]):
                    task[0] = max(task[0], t + GAP)
            tasks.sort(key=lambda e: e[0])
        steps.append(what)
    return steps


def split_dot(a, b):
    high = a.astype(BF)
    rest = (a - high.astype(F32)).astype(BF)
    return jnp.dot(high, b, preferred_element_type=F32) + jnp.dot(rest, b, preferred_element_type=F32)


def iota(shape, axis):
    return lax.broadcasted_iota(jnp.int32, shape, axis)


def one_hot(mask):
    return jnp.where(mask, jnp.float32(1), jnp.float32(0)).astype(BF)


def swap_quads(block):
    row, lane = iota((8, 128), 0) // 4, iota((8, 128), 1) // 32
    far = lane // 2
    top = jnp.where(far == 0, block[:8], pltpu.roll(block[8:], 64, 1))
    bottom = jnp.where(far == 1, block[8:], pltpu.roll(block[:8], 64, 1))
    near = lane & 1
    result = []
    for part in (top, bottom):
        turned = pltpu.roll(part, 4, 0)
        moved = jnp.where(near == 1, pltpu.roll(turned, 32, 1), pltpu.roll(turned, 96, 1))
        result.append(jnp.where(near == row, part, moved))
    return jnp.concatenate(result, 0)


def groups(block, moves):
    return [pltpu.roll(rows, m, 1) if m else rows for rows, m in zip(block, moves)]


def pack(block):
    parts = block[:GR], block[GR : 2 * GR], jnp.concatenate([block[2 * GR :], jnp.zeros((3 * GR - KP, 128), F32)], 0)
    lane = iota((GR, 128), 1)
    halves = []
    for moves in ((0, 40, 80), (88, 0, 40)):
        first, second, third = groups(parts, moves)
        halves.append(jnp.where(lane < 40, first, jnp.where(lane < 80, second, third)))
    return jnp.concatenate(halves, 0)


def unpack(block):
    low, high = block[:GR], block[GR:]
    lane = iota((GR, 128), 1)
    parts = []
    for moves in ((0, 40), (88, 0), (48, 88)):
        first, second = groups((low, high), moves)
        parts.append(jnp.where(lane < 40, first, second))
    return jnp.concatenate([parts[0], parts[1], parts[2][: KP - 2 * GR]], 0)


def kernel(
    x_ref, eo_ref, ev_ref, sum_ref,
    a_buf, slab, s_in, s_all, r_buf, c_buf, c_rx, factor, eacc, row_e, lane_e, msg, rx1, msg2, rx2,
    a_send, a_recv, s_send, s_recv, r_send, r_recv, c_send, c_recv, f_send, f_recv, g_send, g_recv, hello,
):
    w, u = lax.axis_index("virt"), lax.axis_index("aux")
    xx, zz = w // NZ, w % NZ
    yy, core = u // 2, u % 2

    def at_plane(dx, dz):
        return (xx + dx) % NX * NZ + (zz + dz) % NZ

    def at_line(dy, dc):
        return (yy + dy) % NY * 2 + (core + dc) % 2

    barrier = pltpu.get_barrier_semaphore()
    for e in NEXT:
        pl.semaphore_signal(barrier, inc=1, device_id=(at_plane(e // NZ, e % NZ), u), device_id_type=MESH)
    for e in LINE:
        pl.semaphore_signal(barrier, inc=1, device_id=(w, at_line(e // 2, e % 2)), device_id_type=MESH)

    pad = one_hot(iota((KP, ROWS), 0) == iota((KP, ROWS), 1))
    own = jnp.dot(pad, x_ref[...], preferred_element_type=F32).astype(BF)
    for n in range(0, NY, 2):
        lane = iota((AW, 256), 1)
        inner = lane & 127
        upper = jnp.where(inner < 40, 0, 1)
        source = (4 * n + 4 * (lane // 128) + 2 * upper + (inner & 1)) * O + (inner - 40 * upper) // 2
        pick = one_hot((iota((AW, 256), 0) == source) & (inner < SR))
        both = jnp.dot(own, pick, preferred_element_type=F32)
        slab[n] = pack(both[:, :128]).astype(BF)
        slab[n + 1] = pack(both[:, 128:]).astype(BF)
    with jax.named_scope("barrier"):
        pl.semaphore_wait(barrier, len(NEXT) + len(LINE))

    def slab_copy(delta):
        return pltpu.make_async_remote_copy(
            src_ref=slab.at[(yy + NY - delta) % NY], dst_ref=s_in.at[POS[delta]], send_sem=s_send,
            recv_sem=s_recv.at[POS[delta]], device_id=(w, at_line(NY - delta, 0)), device_id_type=MESH,
        )

    def ring_copy(step, delta, h):
        there = (delta + step) % NY
        part = KP // A_PARTS
        return pltpu.make_async_remote_copy(
            src_ref=a_buf.at[pl.ds(POS[delta] * KP + h * part, part)],
            dst_ref=a_buf.at[pl.ds(POS[there] * KP + h * part, part)], send_sem=a_send,
            recv_sem=a_recv.at[POS[there], h], device_id=(w, at_line((NY - step) % NY, 0)), device_id_type=MESH,
        )

    def tree_copy(child, piece):
        parent = TREE[child][piece][0]
        lanes = pl.ds(BOUNDS[piece], BOUNDS[piece + 1] - BOUNDS[piece])
        step = ((parent[0] - child[0]) % NX, (parent[1] - child[1]) % NZ)
        return pltpu.make_async_remote_copy(
            src_ref=r_buf.at[SLOT[parent], :, lanes], dst_ref=r_buf.at[SLOT[child], :, lanes], send_sem=r_send,
            recv_sem=r_recv.at[SLOT[child], piece], device_id=(at_plane(*step), u), device_id_type=MESH,
        )

    for delta in (1, 7, 2, 6, 3, 5, 4):
        slab_copy(delta).start()
    s_all[0:KP] = unpack(slab[yy].astype(F32)).astype(BF)

    row = iota((SR, 128), 0)
    eye = one_hot(iota((SR, 128), 1) == (row // 2 & 1) * 40 + row // 4 * 2 + (row & 1))
    def own_piece(piece):
        lanes = slice(BOUNDS[piece], BOUNDS[piece + 1])
        turned = lax.dot_general(eye, s_all[lanes], (((1,), (1,)), ((), ())), preferred_element_type=F32)
        r_buf[0, :, lanes] = turned.astype(BF)
        for child in passed_on((0, 0), piece):
            tree_copy(child, piece).start()

    def take_slab(pos):
        with jax.named_scope(f"slab_wait{pos}"):
            slab_copy(DELTA[pos]).wait_recv()
        s_all[pos * KP : pos * KP + KP] = unpack(s_in[pos].astype(F32)).astype(BF)
        for piece in range(PIECES):
            if (BOUNDS[piece + 1] - 1) // KP == pos:
                own_piece(piece)
        if pos == A_AFTER:
            for h in range(A_PARTS):
                ring_copy(1, 0, h).start()
                ring_copy(7, 0, h).start()

    if BOUNDS[1] <= KP:
        own_piece(0)

    for first, width in ((0, 256), (256, 256), (512, 128)):
        lane = iota((AW, width), 1) + first
        pick = one_hot(iota((AW, width), 0) == (lane & 31) * O + lane // 32)
        a_buf[0:KP, first : first + width] = jnp.dot(own, pick, preferred_element_type=F32).astype(BF)

    quad_b = iota((8, 128), 0) & 3
    for n in range(O // 2):
        top = iota((8, 128), 0) < 4
        row_e[8 * n : 8 * n + 8] = jnp.where(top, eo_ref[2 * n], eo_ref[2 * n + 1])
    own_v = jnp.zeros((8, 128), F32)
    lane32 = iota((8, 128), 1) & 31
    for a in range(32):
        own_v = jnp.where(lane32 == a, ev_ref[w * 32 + a], own_v)
    for n in range(AW // 128):
        group = iota((8, 128), 1) // 32
        occ = jnp.full((8, 128), eo_ref[4 * n], F32)
        for r in range(1, 4):
            occ = jnp.where(group == r, eo_ref[4 * n + r], occ)
        lane_e[:, 128 * n : 128 * n + 128] = occ - own_v
    eacc[...] = jnp.zeros_like(eacc)
    msg[...] = jnp.zeros_like(msg)

    def core_copy(p):
        return pltpu.make_async_remote_copy(
            src_ref=c_buf.at[p, 1 - core], dst_ref=c_rx.at[p], send_sem=c_send, recv_sem=c_recv.at[p],
            device_id=(w, at_line(0, 1)), device_id_type=MESH,
        )

    seen = {("r", (0, 0), n) for n in range(PIECES)} | {("a", 0, h) for h in range(A_PARTS)}

    def wait_tree(block, piece):
        if ("r", block, piece) not in seen:
            seen.add(("r", block, piece))
            with jax.named_scope(f"r{block[0]}{block[1]}_{piece}"):
                tree_copy(block, piece).wait_recv()
            if piece == 0:
                pl.semaphore_signal(hello, inc=1, device_id=(at_plane(*block), u), device_id_type=MESH)

    def wait_ring(delta, h):
        if ("a", delta, h) not in seen:
            seen.add(("a", delta, h))
            step = 1 if (delta, h) in ring_pieces(1) else 7
            with jax.named_scope(f"a{delta}_{h}"):
                ring_copy(step, (delta - step) % NY, h).wait_recv()

    def multiply(p, first, last):
        pieces, chunks = part_needs(first, last)
        for m in pieces:
            wait_tree(ORDER[2 * p], m)
            wait_tree(ORDER[2 * p + 1], m)
        for m in chunks:
            for h in range(A_PARTS):
                wait_ring(DELTA[m], h)
        part = slice(first, last)
        rows = r_buf[2 * p : 2 * p + 2, :, part].reshape(2 * SR, last - first)
        product = jnp.dot(rows, a_buf[part], preferred_element_type=F32)
        if first == 0:
            c_buf[p, 0] = product[:SR]
            c_buf[p, 1] = product[SR:]
        else:
            c_buf[p, 0] += product[:SR]
            c_buf[p, 1] += product[SR:]
        if last == KK:
            core_copy(p).start()

    def divide(p):
        (x0, z0), (x1, z1) = ORDER[2 * p], ORDER[2 * p + 1]
        other = at_plane(x0 + core * (x1 - x0), z0 + core * (z1 - z0))
        w0, w1 = (0.5 if d in HALF else 1.0 for d in ORDER[2 * p : 2 * p + 2])
        weight = jnp.where(core == 0, jnp.float32(w0), jnp.float32(w1))
        minus = jnp.zeros((8, 128), F32)
        for b in range(NB):
            minus = jnp.where(quad_b == b, ev_ref[other * 32 + yy * NB + b], minus)
        for q in range(10):
            rows = slice(8 * q, 8 * q + 8)
            part = row_e[rows] - minus
            for l in range(5):
                lanes = slice(128 * l, 128 * l + 128)
                factor[p, rows, lanes] = weight / (part + lane_e[:, lanes])

    def finish(p):
        with jax.named_scope(f"c_wait{p}"):
            core_copy(p).wait_recv()
        c_rx[p] = c_rx[p] + c_buf[p, core]
        shares = jnp.zeros((16, 128), F32)
        for q in range(5):
            rows = slice(16 * q, 16 * q + 16)
            for l in range(5):
                lanes = slice(128 * l, 128 * l + 128)
                value = c_rx[p, rows, lanes]
                inner = 2.0 * value
                if l >= q:
                    swapped = swap_quads(c_rx[p, 16 * l : 16 * l + 16, 128 * q : 128 * q + 128])
                    inner = inner - swapped if l == q else 2.0 * (value - swapped)
                term = value * inner * factor[p, rows, lanes]
                eacc[rows, lanes] += term
                shares += term
        shares = shares[:8] + shares[8:]
        total = jnp.sum(shares[:4] + shares[4:], axis=1, keepdims=True)
        msg[...] += jnp.where(iota((4, 128), 1) == 100 + p, total, 0.0)

    for step in program_order():
        if step[0] == "s":
            take_slab(step[1])
        elif step[0] == "a":
            _, way, delta, h = step
            wait_ring(delta, h)
            ring_copy(way, delta, h).start()
        elif step[0] == "r":
            _, block, piece = step
            wait_tree(block, piece)
            for child in passed_on(block, piece):
                tree_copy(child, piece).start()
        else:
            with jax.named_scope("_".join(map(str, step))):
                {"m": multiply, "f": finish, "d": divide}[step[0]](*step[1:])

    total = eacc[...]
    lane = iota((AW, 128), 1)
    pick = one_hot((iota((AW, 128), 0) // 32 == lane % O) & (lane < 5 * O))
    summed = split_dot(total, pick)
    row, lane = iota((SR, 128), 0), iota((SR, 128), 1)
    summed = jnp.where(row // 16 == lane // O, summed, 0.0)
    fold = one_hot(iota((8, SR), 0) == (iota((8, SR), 1) // 4 & 3))
    high = summed.astype(BF)
    rest = (summed - high.astype(F32)).astype(BF)
    packed = jnp.dot(fold, high, preferred_element_type=F32) + jnp.dot(fold, rest, preferred_element_type=F32)
    msg[...] += packed[:4]
    pl.semaphore_wait(hello, NBLK - 1)
    for e in PLANE:
        pltpu.make_async_remote_copy(
            src_ref=msg, dst_ref=rx1.at[e], send_sem=f_send, recv_sem=f_recv,
            device_id=(at_plane(e // NZ, e % NZ), u), device_id_type=MESH,
        ).start()
    own = total[:, 0:128]
    for n in range(1, 5):
        own = own + total[:, 128 * n : 128 * n + 128]
    own = jnp.sum(own, axis=0, keepdims=True)
    own = own + pltpu.roll(own, 64, 1)
    own = own + pltpu.roll(own, 32, 1)
    row, lane = iota((4, 128), 0), iota((4, 128), 1)
    tail = jnp.zeros((4, 128), F32)
    for r in range(4):
        tail = jnp.where(row == r, pltpu.roll(own, 100 - 8 * r, 1), tail)

    def drain(ref, sem):
        pltpu.make_async_copy(ref, ref, sem).wait()

    drain(s_in.at[1:], s_send)
    drain(a_buf.at[KP:], a_send)
    drain(r_buf.at[1:], r_send)
    drain(c_rx, c_send)
    with jax.named_scope("f_wait"):
        pltpu.make_async_copy(rx1.at[1:], rx1.at[1:], f_recv).wait()
    pairs = msg[...]
    theirs = jnp.zeros((4, 128), F32)
    for e in range(NX * NZ):
        got = msg[...] if e == 0 else rx1[e]
        if e:
            pairs = pairs + got
        n = SLOT.get((e // NZ, e % NZ))
        if n is not None:
            theirs = theirs + jnp.where((lane == 100 + n // 2) & (core == n % 2), got, 0.0)
    theirs = jnp.sum(theirs, axis=1, keepdims=True)
    theirs = jnp.where(lane == 100 + (yy & 1) * NB + row, theirs, 0.0)
    theirs = jnp.sum(theirs, axis=0, keepdims=True)
    tail = tail + jnp.where(row == yy // 2, theirs, 0.0)
    msg2[...] = jnp.where(lane < 100, pairs, tail)
    for e in LINE:
        pltpu.make_async_remote_copy(
            src_ref=msg2, dst_ref=rx2.at[e], send_sem=g_send, recv_sem=g_recv,
            device_id=(w, at_line(NY - e // 2, e % 2)), device_id_type=MESH,
        ).start()
    with jax.named_scope("g_wait"):
        pltpu.make_async_copy(rx2.at[1:], rx2.at[1:], g_recv).wait()
    total = msg2[...]
    for e in range(1, 2 * NY):
        total = total + rx2[e]
    sum_ref[...] = total

    drain(rx1.at[1:], f_send)
    drain(rx2.at[1:], g_send)


def open_sums(sum_ref, virt_ref, pair_ref, square):
    total = sum_ref[...]
    row, lane = iota((4, 128), 0), iota((4, 128), 1)
    line = jnp.zeros((4, 128), F32)
    for r in range(4):
        line = jnp.where((row == r) & (lane // 8 == r), pltpu.roll(total, 28 + 8 * r, 1), line)
    virt_ref[...] = jnp.sum(line, axis=0)[:32]
    square[...] = jnp.zeros_like(square)
    for q in range(5):
        square[4 * q : 4 * q + 4] = pltpu.roll(total, (128 - O * q) % 128, 1)
    wide = square[...]
    pair_ref[...] = (wide + jnp.transpose(wide))[:O, :O]


def on_device(three_index, eps_occ, eps_virt):
    vmem, smem = pl.BlockSpec(memory_space=pltpu.VMEM), pl.BlockSpec(memory_space=pltpu.SMEM)
    dma = pltpu.SemaphoreType.DMA
    sums = pl.pallas_call(
        kernel,
        out_shape=jax.ShapeDtypeStruct((4, 128), F32),
        in_specs=[vmem, smem, smem],
        out_specs=vmem,
        scratch_shapes=[
            pltpu.VMEM((KK, AW), BF),
            pltpu.VMEM((NY, 2 * GR, 128), BF),
            pltpu.VMEM((NY, 2 * GR, 128), BF),
            pltpu.VMEM((KK, 128), BF),
            pltpu.VMEM((NBLK, SR, KK), BF),
            pltpu.VMEM((NPAIR, 2, SR, AW), F32),
            pltpu.VMEM((NPAIR, SR, AW), F32),
            pltpu.VMEM((NPAIR, SR, AW), F32),
            pltpu.VMEM((SR, AW), F32),
            pltpu.VMEM((SR, 128), F32),
            pltpu.VMEM((8, AW), F32),
            pltpu.VMEM((4, 128), F32),
            pltpu.VMEM((NX * NZ, 4, 128), F32),
            pltpu.VMEM((4, 128), F32),
            pltpu.VMEM((2 * NY, 4, 128), F32),
            dma, dma((NY, A_PARTS)), dma, dma((NY,)), dma, dma((NBLK, PIECES)), dma, dma((NPAIR,)),
            dma, dma, dma, dma, pltpu.SemaphoreType.REGULAR,
        ],
        compiler_params=pltpu.CompilerParams(collective_id=0, has_side_effects=True, vmem_limit_bytes=56 * 1024 * 1024),
        name="mp2",
    )(three_index, eps_occ, eps_virt)
    return pl.pallas_call(
        open_sums,
        out_shape=(jax.ShapeDtypeStruct((32,), F32), jax.ShapeDtypeStruct((O, O), F32)),
        in_specs=[vmem],
        out_specs=(vmem, vmem),
        scratch_shapes=[pltpu.VMEM((128, 128), F32)],
        name="sums",
    )(sums)


def solution(mesh):
    return jax.shard_map(
        on_device, mesh=mesh, in_specs=(P("aux", "virt"), P(), P()), out_specs=(P("virt"), P()), check_vma=False
    )
```

```python
import jax
import jax.numpy as jnp
from jax import lax
from jax.experimental import pallas as pl
from jax.experimental.pallas import tpu as pltpu
from jax.sharding import PartitionSpec as P

MESH = pl.DeviceIdType.MESH
BF = jnp.bfloat16
F32 = jnp.float32

O = 20
VIRT = 1024
NX, NY, NZ = 4, 8, 8
ROWS, KP = 150, 160
AW = 640
NB = 4
SR = NB * O
KK = NY * KP
GR = 56
ORDER = (
    (0, 0), (1, 0), (0, 1), (3, 1), (2, 0), (0, 2), (2, 7), (3, 2), (0, 3),
    (2, 6), (3, 7), (3, 3), (0, 4), (2, 5), (3, 6), (3, 4), (2, 4), (3, 5),
)
SLOT = {d: n for n, d in enumerate(ORDER)}
HALF = ((0, 0), (0, 4), (2, 0), (2, 4))
NBLK = len(ORDER)
NPAIR = NBLK // 2
TREE = {
    (1, 0): (((0, 0), 6.8), ((0, 0), 9.2), ((0, 0), 11.0), ((0, 0), 13.2), ((0, 0), 14.1)),
    (0, 1): (((0, 0), 6.8), ((0, 0), 9.2), ((0, 0), 11.0), ((0, 0), 13.2), ((0, 0), 15.0)),
    (3, 1): (((3, 2), 17.2), ((0, 1), 12.3), ((0, 1), 14.1), ((0, 1), 16.3), ((0, 1), 18.1)),
    (2, 0): (((1, 0), 10.1), ((1, 0), 12.3), ((1, 0), 15.0), ((1, 0), 16.3), ((1, 0), 18.1)),
    (0, 2): (((0, 1), 10.1), ((0, 1), 12.3), ((0, 1), 15.9), ((0, 1), 17.7), ((0, 1), 18.6)),
    (2, 7): (((2, 0), 13.2), ((2, 0), 15.4), ((2, 0), 18.1), ((2, 0), 19.9), ((2, 0), 21.2)),
    (3, 2): (((0, 2), 13.2), ((0, 2), 15.4), ((0, 2), 19.0), ((0, 2), 20.8), ((0, 2), 21.7)),
    (0, 3): (((0, 2), 14.1), ((0, 2), 16.8), ((0, 2), 19.5), ((0, 2), 21.3), ((0, 2), 22.2)),
    (2, 6): (((2, 7), 16.3), ((2, 7), 19.0), ((2, 7), 22.1), ((2, 7), 23.0), ((2, 7), 24.3)),
    (3, 7): (((2, 7), 17.2), ((2, 7), 19.0), ((2, 7), 21.2), ((2, 7), 23.0), ((2, 7), 24.8)),
    (3, 3): (((0, 3), 17.2), ((0, 3), 19.9), ((0, 3), 22.6), ((0, 3), 24.4), ((0, 3), 25.3)),
    (0, 4): (((3, 4), 23.9), ((3, 4), 27.5), ((0, 3), 23.1), ((0, 3), 25.8), ((0, 3), 26.7)),
    (2, 5): (((3, 5), 28.0), ((2, 4), 30.2), ((2, 6), 25.2), ((2, 6), 26.1), ((2, 6), 27.4)),
    (3, 6): (((2, 6), 19.9), ((2, 6), 22.1), ((2, 6), 25.7), ((2, 6), 26.6), ((3, 7), 28.3)),
    (3, 4): (((3, 3), 20.4), ((3, 3), 24.0), ((0, 4), 26.2), ((0, 4), 28.9), ((3, 3), 28.5)),
    (2, 4): (((3, 4), 23.5), ((3, 4), 27.1), ((3, 4), 29.8), ((2, 5), 29.2), ((2, 5), 30.5)),
    (3, 5): (((3, 4), 24.9), ((3, 4), 27.6), ((2, 5), 28.4), ((2, 5), 29.3), ((2, 5), 30.5)),
}
BOUNDS = (0, 256, 512, 768, 1024, 1280)
PIECES = len(BOUNDS) - 1
POS = {0: 0, 1: 1, 7: 2, 2: 3, 6: 4, 3: 5, 5: 6, 4: 7}
DELTA = {n: d for d, n in POS.items()}
PARTS = (0, 768, KK)
A_AFTER = 3
A_PARTS = 5
LATE, SLACK, GAP = 0.7, 0.5, 3.5
SLABS = (0.0, 3.3, 4.2, 5.8, 6.8, 8.5, 8.9, 9.8)

RING = {
    1: (8.9, 9.8, 10.7, 11.6, 12.5, 13.4, 14.3, 15.2, 16.1, 17.0, 17.9, 18.8, 19.7, 20.6, 21.5, 22.4, 23.3, 24.2),
    7: (8.9, 9.8, 10.7, 11.6, 12.5, 13.4, 14.3, 15.2, 16.1, 17.0, 17.9, 18.8, 19.7, 20.6, 21.5, 22.4, 23.3),
}


def hops(dx, dz, dy):
    return min(dx, NX - dx) + min(dz, NZ - dz) + min(dy, NY - dy)


PLANE = sorted(range(1, NX * NZ), key=lambda e: -hops(e // NZ, e % NZ, 0))
NEXT = [e for e in PLANE if hops(e // NZ, e % NZ, 0) == 1]
LINE = sorted(range(1, 2 * NY), key=lambda e: -hops(0, 0, e // 2))


def passed_on(block, piece):
    return [child for child, row in TREE.items() if row[piece][0] == block]


def ring_pieces(step):
    last = range(3) if step == 1 else range(3, A_PARTS)
    return [(step * n % NY, h) for n in range(1, 4) for h in range(A_PARTS)] + [(4, h) for h in last]


def ring_goes_on(step, delta, h):
    return ((delta + step) % NY, h) in ring_pieces(step)


def part_needs(first, last):
    pieces = [m for m in range(PIECES) if BOUNDS[m] < last and BOUNDS[m + 1] > first]
    return pieces, range(first // KP, (last - 1) // KP + 1)


def program_order():
    forward, arrival = [], {((0, 0), n): 0.0 for n in range(PIECES)}
    for block, row in TREE.items():
        for piece, (_, t) in enumerate(row):
            arrival[block, piece] = t
            if piece == 0 or passed_on(block, piece):
                forward.append((t, ("r", block, piece)))
    forward += [(t, ("s", pos)) for pos, t in enumerate(SLABS) if pos]
    rings = {}
    for step, times in RING.items():
        for (delta, h), t in zip(ring_pieces(step), times):
            rings[delta, h] = t
            if ring_goes_on(step, delta, h):
                forward.append((t, ("a", step, delta, h)))
    forward.sort(key=lambda e: e[0])
    tasks = [[0.0, 0.25, ("d", p)] for p in range(NPAIR)]
    last = max(rings.values())
    for p in range(NPAIR):
        both = ORDER[2 * p : 2 * p + 2]
        early = max(arrival[b, m] for b in both for m in range(PIECES)) < last - 1.0
        bounds = PARTS if early else (0, KK)
        ready = 0.0
        for a, b in zip(bounds, bounds[1:]):
            pieces, chunks = part_needs(a, b)
            times = [arrival[d, m] for d in both for m in pieces]
            times += [rings[DELTA[m], h] for m in chunks if m for h in range(A_PARTS)]
            ready = max([ready] + times)
            tasks.append([ready + LATE, 0.2 + 0.25 * (b - a) / KK, ("m", p, a, b)])
        tasks.append([ready + LATE + GAP, 0.25, ("f", p)])
    tasks.sort(key=lambda e: e[0])
    steps, t = [], 0.0
    while forward or tasks:
        if not tasks or forward and max(t, tasks[0][0]) + tasks[0][1] > forward[0][0] + SLACK:
            when, what = forward.pop(0)
            t = max(t, when)
        else:
            ready, length, what = tasks.pop(0)
            t = max(t, ready) + length
            for task in tasks:
                if what[0] == "m" and task[2] == ("f", what[1]):
                    task[0] = max(task[0], t + GAP)
            tasks.sort(key=lambda e: e[0])
        steps.append(what)
    return steps


def split_dot(a, b):
    high = a.astype(BF)
    rest = (a - high.astype(F32)).astype(BF)
    return jnp.dot(high, b, preferred_element_type=F32) + jnp.dot(rest, b, preferred_element_type=F32)


def iota(shape, axis):
    return lax.broadcasted_iota(jnp.int32, shape, axis)


def one_hot(mask):
    return jnp.where(mask, jnp.float32(1), jnp.float32(0)).astype(BF)


def swap_quads(block):
    row, lane = iota((8, 128), 0) // 4, iota((8, 128), 1) // 32
    far = lane // 2
    top = jnp.where(far == 0, block[:8], pltpu.roll(block[8:], 64, 1))
    bottom = jnp.where(far == 1, block[8:], pltpu.roll(block[:8], 64, 1))
    near = lane & 1
    result = []
    for part in (top, bottom):
        turned = pltpu.roll(part, 4, 0)
        moved = jnp.where(near == 1, pltpu.roll(turned, 32, 1), pltpu.roll(turned, 96, 1))
        result.append(jnp.where(near == row, part, moved))
    return jnp.concatenate(result, 0)


def groups(block, moves):
    return [pltpu.roll(rows, m, 1) if m else rows for rows, m in zip(block, moves)]


def pack(block):
    parts = block[:GR], block[GR : 2 * GR], jnp.concatenate([block[2 * GR :], jnp.zeros((3 * GR - KP, 128), F32)], 0)
    lane = iota((GR, 128), 1)
    halves = []
    for moves in ((0, 40, 80), (88, 0, 40)):
        first, second, third = groups(parts, moves)
        halves.append(jnp.where(lane < 40, first, jnp.where(lane < 80, second, third)))
    return jnp.concatenate(halves, 0)


def unpack(block):
    low, high = block[:GR], block[GR:]
    lane = iota((GR, 128), 1)
    parts = []
    for moves in ((0, 40), (88, 0), (48, 88)):
        first, second = groups((low, high), moves)
        parts.append(jnp.where(lane < 40, first, second))
    return jnp.concatenate([parts[0], parts[1], parts[2][: KP - 2 * GR]], 0)


def kernel(
    x_hbm, eo_hbm, ev_hbm, sum_ref, x_ref, eo_ref, ev_ref, in_sem,
    a_buf, slab, s_in, s_all, r_buf, c_buf, c_rx, factor, eacc, row_e, lane_e, msg, rx1, msg2, rx2, gather,
    a_send, a_recv, s_send, s_recv, r_send, r_recv, c_send, c_recv, f_send, f_recv, g_send, g_recv, hello,
):
    inputs = [
        pltpu.make_async_copy(given, here, in_sem.at[n])
        for n, (given, here) in enumerate(((x_hbm, x_ref), (eo_hbm, eo_ref), (ev_hbm, ev_ref)))
    ]
    for copy in inputs:
        copy.start()
    w, u = lax.axis_index("virt"), lax.axis_index("aux")
    xx, zz = w // NZ, w % NZ
    yy, core = u // 2, u % 2

    def at_plane(dx, dz):
        return (xx + dx) % NX * NZ + (zz + dz) % NZ

    def at_line(dy, dc):
        return (yy + dy) % NY * 2 + (core + dc) % 2

    barrier = pltpu.get_barrier_semaphore()
    for e in NEXT:
        pl.semaphore_signal(barrier, inc=1, device_id=(at_plane(e // NZ, e % NZ), u), device_id_type=MESH)
    for e in LINE:
        pl.semaphore_signal(barrier, inc=1, device_id=(w, at_line(e // 2, e % 2)), device_id_type=MESH)

    pad = one_hot(iota((KP, ROWS), 0) == iota((KP, ROWS), 1))
    inputs[0].wait()
    own = jnp.dot(pad, x_ref[...], preferred_element_type=F32).astype(BF)
    for n in range(0, NY, 2):
        lane = iota((1, 256), 1)
        inner = lane & 127
        upper = jnp.where(inner < 40, 0, 1)
        source = (4 * n + 4 * (lane // 128) + 2 * upper + (inner & 1)) * O + (inner - 40 * upper) // 2
        pick = one_hot(iota((AW, 256), 0) == jnp.where(inner < SR, source, -1))
        both = jnp.dot(own, pick, preferred_element_type=F32)
        slab[n] = pack(both[:, :128]).astype(BF)
        slab[n + 1] = pack(both[:, 128:]).astype(BF)
    with jax.named_scope("barrier"):
        pl.semaphore_wait(barrier, len(NEXT) + len(LINE))

    def slab_copy(delta):
        return pltpu.make_async_remote_copy(
            src_ref=slab.at[(yy + NY - delta) % NY], dst_ref=s_in.at[POS[delta]], send_sem=s_send,
            recv_sem=s_recv.at[POS[delta]], device_id=(w, at_line(NY - delta, 0)), device_id_type=MESH,
        )

    def ring_copy(step, delta, h):
        there = (delta + step) % NY
        part = KP // A_PARTS
        return pltpu.make_async_remote_copy(
            src_ref=a_buf.at[pl.ds(POS[delta] * KP + h * part, part)],
            dst_ref=a_buf.at[pl.ds(POS[there] * KP + h * part, part)], send_sem=a_send,
            recv_sem=a_recv.at[POS[there], h], device_id=(w, at_line((NY - step) % NY, 0)), device_id_type=MESH,
        )

    def tree_copy(child, piece):
        parent = TREE[child][piece][0]
        lanes = pl.ds(BOUNDS[piece], BOUNDS[piece + 1] - BOUNDS[piece])
        step = ((parent[0] - child[0]) % NX, (parent[1] - child[1]) % NZ)
        return pltpu.make_async_remote_copy(
            src_ref=r_buf.at[SLOT[parent], :, lanes], dst_ref=r_buf.at[SLOT[child], :, lanes], send_sem=r_send,
            recv_sem=r_recv.at[SLOT[child], piece], device_id=(at_plane(*step), u), device_id_type=MESH,
        )

    for delta in (1, 7, 2, 6, 3, 5, 4):
        slab_copy(delta).start()
    s_all[0:KP] = unpack(slab[yy].astype(F32)).astype(BF)

    row = iota((SR, 128), 0)
    eye = one_hot(iota((SR, 128), 1) == (row // 2 & 1) * 40 + row // 4 * 2 + (row & 1))
    def own_piece(piece):
        lanes = slice(BOUNDS[piece], BOUNDS[piece + 1])
        turned = lax.dot_general(eye, s_all[lanes], (((1,), (1,)), ((), ())), preferred_element_type=F32)
        r_buf[0, :, lanes] = turned.astype(BF)
        for child in passed_on((0, 0), piece):
            tree_copy(child, piece).start()

    def take_slab(pos):
        with jax.named_scope(f"slab_wait{pos}"):
            slab_copy(DELTA[pos]).wait_recv()
        s_all[pos * KP : pos * KP + KP] = unpack(s_in[pos].astype(F32)).astype(BF)
        for piece in range(PIECES):
            if (BOUNDS[piece + 1] - 1) // KP == pos:
                own_piece(piece)
        if pos == A_AFTER:
            for h in range(A_PARTS):
                ring_copy(1, 0, h).start()
                ring_copy(7, 0, h).start()

    if BOUNDS[1] <= KP:
        own_piece(0)

    for first, width in ((0, 256), (256, 256), (512, 128)):
        lane = iota((1, width), 1) + first
        pick = one_hot(iota((AW, width), 0) == (lane & 31) * O + lane // 32)
        a_buf[0:KP, first : first + width] = jnp.dot(own, pick, preferred_element_type=F32).astype(BF)

    inputs[1].wait()
    inputs[2].wait()
    quad_b = iota((8, 128), 0) & 3
    for n in range(O // 2):
        top = iota((8, 128), 0) < 4
        row_e[8 * n : 8 * n + 8] = jnp.where(top, eo_ref[2 * n], eo_ref[2 * n + 1])
    own_v = jnp.zeros((8, 128), F32)
    lane32 = iota((8, 128), 1) & 31
    for a in range(32):
        own_v = jnp.where(lane32 == a, ev_ref[w * 32 + a], own_v)
    for n in range(AW // 128):
        group = iota((8, 128), 1) // 32
        occ = jnp.full((8, 128), eo_ref[4 * n], F32)
        for r in range(1, 4):
            occ = jnp.where(group == r, eo_ref[4 * n + r], occ)
        lane_e[:, 128 * n : 128 * n + 128] = occ - own_v
    lane = iota((1, 128), 1)
    gather[...] = one_hot(iota((AW, 128), 0) // 32 == jnp.where(lane < 5 * O, lane % O, -1))
    eacc[...] = jnp.zeros_like(eacc)
    msg[...] = jnp.zeros_like(msg)

    def core_copy(p):
        return pltpu.make_async_remote_copy(
            src_ref=c_buf.at[p, 1 - core], dst_ref=c_rx.at[p], send_sem=c_send, recv_sem=c_recv.at[p],
            device_id=(w, at_line(0, 1)), device_id_type=MESH,
        )

    seen = {("r", (0, 0), n) for n in range(PIECES)} | {("a", 0, h) for h in range(A_PARTS)}

    def wait_tree(block, piece):
        if ("r", block, piece) not in seen:
            seen.add(("r", block, piece))
            with jax.named_scope(f"r{block[0]}{block[1]}_{piece}"):
                tree_copy(block, piece).wait_recv()
            if piece == 0:
                pl.semaphore_signal(hello, inc=1, device_id=(at_plane(*block), u), device_id_type=MESH)

    def wait_ring(delta, h):
        if ("a", delta, h) not in seen:
            seen.add(("a", delta, h))
            step = 1 if (delta, h) in ring_pieces(1) else 7
            with jax.named_scope(f"a{delta}_{h}"):
                ring_copy(step, (delta - step) % NY, h).wait_recv()

    def multiply(p, first, last):
        pieces, chunks = part_needs(first, last)
        for m in pieces:
            wait_tree(ORDER[2 * p], m)
            wait_tree(ORDER[2 * p + 1], m)
        for m in chunks:
            for h in range(A_PARTS):
                wait_ring(DELTA[m], h)
        part = slice(first, last)
        rows = r_buf[2 * p : 2 * p + 2, :, part].reshape(2 * SR, last - first)
        product = jnp.dot(rows, a_buf[part], preferred_element_type=F32)
        if first == 0:
            c_buf[p, 0] = product[:SR]
            c_buf[p, 1] = product[SR:]
        else:
            c_buf[p, 0] += product[:SR]
            c_buf[p, 1] += product[SR:]
        if last == KK:
            core_copy(p).start()

    def divide(p):
        (x0, z0), (x1, z1) = ORDER[2 * p], ORDER[2 * p + 1]
        other = at_plane(x0 + core * (x1 - x0), z0 + core * (z1 - z0))
        w0, w1 = (0.5 if d in HALF else 1.0 for d in ORDER[2 * p : 2 * p + 2])
        weight = jnp.where(core == 0, jnp.float32(w0), jnp.float32(w1))
        minus = jnp.zeros((8, 128), F32)
        for b in range(NB):
            minus = jnp.where(quad_b == b, ev_ref[other * 32 + yy * NB + b], minus)
        for q in range(10):
            rows = slice(8 * q, 8 * q + 8)
            part = row_e[rows] - minus
            for l in range(5):
                lanes = slice(128 * l, 128 * l + 128)
                factor[p, rows, lanes] = weight / (part + lane_e[:, lanes])

    def finish(p):
        with jax.named_scope(f"c_wait{p}"):
            core_copy(p).wait_recv()
        c_rx[p] = c_rx[p] + c_buf[p, core]
        shares = jnp.zeros((16, 128), F32)
        for q in range(5):
            rows = slice(16 * q, 16 * q + 16)
            for l in range(5):
                lanes = slice(128 * l, 128 * l + 128)
                value = c_rx[p, rows, lanes]
                inner = 2.0 * value
                if l >= q:
                    swapped = swap_quads(c_rx[p, 16 * l : 16 * l + 16, 128 * q : 128 * q + 128])
                    inner = inner - swapped if l == q else 2.0 * (value - swapped)
                term = value * inner * factor[p, rows, lanes]
                eacc[rows, lanes] += term
                shares += term
        shares = shares[:8] + shares[8:]
        total = jnp.sum(shares[:4] + shares[4:], axis=1, keepdims=True)
        msg[...] += jnp.where(iota((4, 128), 1) == 100 + p, total, 0.0)

    for step in program_order():
        if step[0] == "s":
            take_slab(step[1])
        elif step[0] == "a":
            _, way, delta, h = step
            wait_ring(delta, h)
            ring_copy(way, delta, h).start()
        elif step[0] == "r":
            _, block, piece = step
            wait_tree(block, piece)
            for child in passed_on(block, piece):
                tree_copy(child, piece).start()
        else:
            with jax.named_scope("_".join(map(str, step))):
                {"m": multiply, "f": finish, "d": divide}[step[0]](*step[1:])

    total = eacc[...]
    summed = split_dot(total, gather[...])
    row, lane = iota((SR, 128), 0), iota((SR, 128), 1)
    summed = jnp.where(row // 16 == lane // O, summed, 0.0)
    fold = one_hot(iota((8, SR), 0) == (iota((8, SR), 1) // 4 & 3))
    high = summed.astype(BF)
    rest = (summed - high.astype(F32)).astype(BF)
    packed = jnp.dot(fold, high, preferred_element_type=F32) + jnp.dot(fold, rest, preferred_element_type=F32)
    msg[...] += packed[:4]
    pl.semaphore_wait(hello, NBLK - 1)
    for e in PLANE:
        pltpu.make_async_remote_copy(
            src_ref=msg, dst_ref=rx1.at[e], send_sem=f_send, recv_sem=f_recv,
            device_id=(at_plane(e // NZ, e % NZ), u), device_id_type=MESH,
        ).start()
    own = total[:, 0:128]
    for n in range(1, 5):
        own = own + total[:, 128 * n : 128 * n + 128]
    own = jnp.sum(own, axis=0, keepdims=True)
    own = own + pltpu.roll(own, 64, 1)
    own = own + pltpu.roll(own, 32, 1)
    row, lane = iota((4, 128), 0), iota((4, 128), 1)
    tail = jnp.zeros((4, 128), F32)
    for r in range(4):
        tail = jnp.where(row == r, pltpu.roll(own, 100 - 8 * r, 1), tail)

    def drain(ref, sem):
        pltpu.make_async_copy(ref, ref, sem).wait()

    drain(s_in.at[1:], s_send)
    drain(a_buf.at[KP:], a_send)
    drain(r_buf.at[1:], r_send)
    drain(c_rx, c_send)
    with jax.named_scope("f_wait"):
        pltpu.make_async_copy(rx1.at[1:], rx1.at[1:], f_recv).wait()
    pairs = msg[...]
    theirs = jnp.zeros((4, 128), F32)
    for e in range(NX * NZ):
        got = msg[...] if e == 0 else rx1[e]
        if e:
            pairs = pairs + got
        n = SLOT.get((e // NZ, e % NZ))
        if n is not None:
            theirs = theirs + jnp.where((lane == 100 + n // 2) & (core == n % 2), got, 0.0)
    theirs = jnp.sum(theirs, axis=1, keepdims=True)
    theirs = jnp.where(lane == 100 + (yy & 1) * NB + row, theirs, 0.0)
    theirs = jnp.sum(theirs, axis=0, keepdims=True)
    tail = tail + jnp.where(row == yy // 2, theirs, 0.0)
    msg2[...] = jnp.where(lane < 100, pairs, tail)
    for e in LINE:
        pltpu.make_async_remote_copy(
            src_ref=msg2, dst_ref=rx2.at[e], send_sem=g_send, recv_sem=g_recv,
            device_id=(w, at_line(NY - e // 2, e % 2)), device_id_type=MESH,
        ).start()
    with jax.named_scope("g_wait"):
        pltpu.make_async_copy(rx2.at[1:], rx2.at[1:], g_recv).wait()
    total = msg2[...]
    for e in range(1, 2 * NY):
        total = total + rx2[e]
    sum_ref[...] = total

    drain(rx1.at[1:], f_send)
    drain(rx2.at[1:], g_send)


def open_sums(sum_ref, virt_ref, pair_ref, square):
    total = sum_ref[...]
    row, lane = iota((4, 128), 0), iota((4, 128), 1)
    line = jnp.zeros((4, 128), F32)
    for r in range(4):
        line = jnp.where((row == r) & (lane // 8 == r), pltpu.roll(total, 28 + 8 * r, 1), line)
    virt_ref[...] = jnp.sum(line, axis=0)[:32]
    square[...] = jnp.zeros_like(square)
    for q in range(5):
        square[4 * q : 4 * q + 4] = pltpu.roll(total, (128 - O * q) % 128, 1)
    wide = square[...]
    pair_ref[...] = (wide + jnp.transpose(wide))[:O, :O]


def on_device(three_index, eps_occ, eps_virt):
    vmem = pl.BlockSpec(memory_space=pltpu.VMEM)
    dma = pltpu.SemaphoreType.DMA
    sums = pl.pallas_call(
        kernel,
        out_shape=jax.ShapeDtypeStruct((4, 128), F32),
        in_specs=[pl.BlockSpec(memory_space=pl.ANY)] * 3,
        out_specs=vmem,
        scratch_shapes=[
            pltpu.VMEM((ROWS, AW), BF),
            pltpu.SMEM((O,), F32),
            pltpu.SMEM((VIRT,), F32),
            dma((3,)),
            pltpu.VMEM((KK, AW), BF),
            pltpu.VMEM((NY, 2 * GR, 128), BF),
            pltpu.VMEM((NY, 2 * GR, 128), BF),
            pltpu.VMEM((KK, 128), BF),
            pltpu.VMEM((NBLK, SR, KK), BF),
            pltpu.VMEM((NPAIR, 2, SR, AW), F32),
            pltpu.VMEM((NPAIR, SR, AW), F32),
            pltpu.VMEM((NPAIR, SR, AW), F32),
            pltpu.VMEM((SR, AW), F32),
            pltpu.VMEM((SR, 128), F32),
            pltpu.VMEM((8, AW), F32),
            pltpu.VMEM((4, 128), F32),
            pltpu.VMEM((NX * NZ, 4, 128), F32),
            pltpu.VMEM((4, 128), F32),
            pltpu.VMEM((2 * NY, 4, 128), F32),
            pltpu.VMEM((AW, 128), BF),
            dma, dma((NY, A_PARTS)), dma, dma((NY,)), dma, dma((NBLK, PIECES)), dma, dma((NPAIR,)),
            dma, dma, dma, dma, pltpu.SemaphoreType.REGULAR,
        ],
        compiler_params=pltpu.CompilerParams(collective_id=0, has_side_effects=True, vmem_limit_bytes=56 * 1024 * 1024),
        name="mp2",
    )(three_index, eps_occ, eps_virt)
    return pl.pallas_call(
        open_sums,
        out_shape=(jax.ShapeDtypeStruct((32,), F32), jax.ShapeDtypeStruct((O, O), F32)),
        in_specs=[vmem],
        out_specs=(vmem, vmem),
        scratch_shapes=[pltpu.VMEM((128, 128), F32)],
        name="sums",
    )(sums)


def solution(mesh):
    return jax.shard_map(
        on_device, mesh=mesh, in_specs=(P("aux", "virt"), P(), P()), out_specs=(P("virt"), P()), check_vma=False
    )
```
